512 devices in a mesh: blk: 64 (over y_lo, z, core), par: 8 (over x, y_hi).
Axes of the slice: x: 4, y: 8 (y_hi: 2, y_lo: 4; y = y_hi * 4 + y_lo), z: 8, core: 2. Of those that a mesh axis runs over, the one named last changes fastest.
Arguments:
- logder: float32 [8192, 6144], P('blk', 'par'), may hold values from -50 to 50
Outputs:
- kernel_tiles: float32 [64, 33, 128, 128], P('blk', None, 'par')
The draws below stay inside these ranges and needn't reach their ends.
All inputs are finite; a program needn't handle non-finite values.
Results may differ from the reference program's by a relative error of at most 0.00015.
Values sent between devices are 32-bit elements; how exact they have to be, the bound alone decides.
A program may use at most 64 MiB of HBM per device.

```python
import math
import jax
import jax.numpy as jnp
from jax import lax

BS = 128
P_SIZE = 6144
NS = 8192
TILES = 33
N_BLK = 64


def draw_logder(key, part):
    keys = jax.random.split(jax.random.fold_in(key, 7), 4)
    row_scale = jnp.exp(jax.random.uniform(keys[0], (NS, 1), jnp.float32, math.log(0.3), math.log(3.0)))
    col_scale = jnp.exp(jax.random.uniform(keys[1], (1, P_SIZE), jnp.float32, math.log(0.5), math.log(2.0)))
    offset = 1.5 * jax.random.truncated_normal(keys[3], -4.0, 4.0, (1, P_SIZE), jnp.float32)
    ramp = 1.0 + 2.0 * jnp.arange(NS, dtype=jnp.float32)[:, None] / NS
    noise = jax.random.truncated_normal(keys[2], -5.0, 5.0, (NS, P_SIZE), jnp.float32)
    return row_scale * col_scale * noise + offset * ramp


def setup_inputs(seed: int = 0) -> dict:
    seeds = jax.random.split(jax.random.key(seed), 2)
    return {
        "logder": draw_logder(jax.random.fold_in(seeds[1], 71), 0),
    }


def reference(logder):
    mean = jnp.sum(logder, axis=0) / NS
    centered = logder - mean[None, :]
    blocks = centered.reshape(N_BLK, BS, P_SIZE)

    def one_block(index):
        rows = lax.dynamic_index_in_dim(blocks, index, 0, keepdims=False)
        columns = jnp.roll(blocks, -index, axis=0)[:TILES]
        return jnp.einsum("rp,dcp->drc", rows, columns, precision=lax.Precision.HIGHEST) / P_SIZE

    return lax.map(one_block, jnp.arange(N_BLK, dtype=jnp.int32))
```

```python
import jax
import jax.numpy as jnp
from jax import lax
from jax.experimental import pallas as pl
from jax.experimental.pallas import tpu as pltpu
from jax.sharding import Mesh
from jax.sharding import PartitionSpec as P

MESH = pl.DeviceIdType.MESH

ROWS, WIDTH = 128, 768
LANES = 128
COLS = WIDTH // LANES
NCH = 4
CH = ROWS // NCH
NB = 64
HALF = 32
NSAMPLES = 8192
NPARAMS = 6144

NSLOT = 12
UP = {1: 5, 2: 6, 3: 7, 4: 8}
DOWN = {1: 9, 2: 10, 3: 11}

GROUPS = [(0, 6), (6, 8), (14, 8), (22, 8), (30, 5)]
NTILE = 35


def rem(value, count):
    return lax.rem(value, jnp.int32(count))


def div(value, count):
    return lax.div(value, jnp.int32(count))


def kernel(
    x_ref, out_ref, raw, hi, lo, zs, zt, ys, mean, pk, pr, sx, xr, fb,
    own_send, y_send, y_recv, z_send, z_own, z_recv, ms_send, ms_recv, mt_send, mt_recv,
    d_send, d_recv, x_send, x_recv, f_send, f_recv,
):
    a = lax.axis_index("a")
    z = lax.axis_index("z")
    c = lax.axis_index("c")
    x = lax.axis_index("x")
    h = lax.axis_index("h")
    y = h * 4 + a
    first = c == h
    other = c != h

    def at_y(steps, core):
        yy = rem(y + 8 + steps, 8)
        return (rem(yy, 4), z, core, x, div(yy, 4))

    def at_z(steps):
        return (a, rem(z + 8 + steps, 8), c, x, h)

    def at_x(steps):
        return (a, z, c, rem(x + steps, 4), h)

    partner = (a, z, 1 - c, x, h)

    def remote(src, dst, send, recv, device):
        return pltpu.make_async_remote_copy(
            src_ref=src, dst_ref=dst, send_sem=send, recv_sem=recv,
            device_id=device, device_id_type=MESH,
        )

    def landed(ref, sem):
        pltpu.make_async_copy(ref, ref, sem).wait()

    barrier = pltpu.get_barrier_semaphore()

    def hello(device):
        pl.semaphore_signal(barrier, inc=1, device_id=device, device_id_type=MESH)

    hello(partner)
    for k in range(1, 8):
        hello(at_z(k))
        hello(at_y(k, 0))
        hello(at_y(k, 1))
    for k in range(1, 4):
        hello(at_x(k))
    pl.semaphore_wait(barrier, 25)

    def part(i):
        return pl.ds(pl.multiple_of(i * CH, CH), CH)

    def from_below(r):
        return div(rem(y + 8 - r, 8), 4) == c

    def y_own_up(i):
        return remote(x_ref.at[part(i)], raw.at[1, part(i)], own_send.at[0, i], y_recv.at[1, i], at_y(1, c))

    def y_own_down(i):
        return remote(
            x_ref.at[part(i)], raw.at[3, part(i)], own_send.at[0, i], y_recv.at[3, i], at_y(-1, 1 - c)
        )

    def y_own_partner(i):
        return remote(x_ref.at[part(i)], raw.at[4, part(i)], own_send.at[1, i], y_recv.at[4, i], partner)

    def y_relay(r, up, i):
        to = r + 1 if up else r - 1
        return remote(
            raw.at[r, part(i)], raw.at[to, part(i)], y_send.at[r, i], y_recv.at[to, i],
            at_y(1 if up else -1, c),
        )

    def z_start(src, i, low):
        to = UP[1] if low else DOWN[1]
        return remote(
            src.at[part(i)], raw.at[to, part(i)], z_own.at[0 if low else 1, i], z_recv.at[to - 5, i],
            at_z(-1 if low else 1),
        )

    def z_relay(slot, to, i, low):
        return remote(
            raw.at[slot, part(i)], raw.at[to, part(i)], z_send.at[slot - 5, i], z_recv.at[to - 5, i],
            at_z(-1 if low else 1),
        )

    def y_event(dist, i):
        @pl.when(from_below(dist))
        def _():
            landed(raw.at[dist, part(i)], y_recv.at[dist, i])
            if dist < 4:
                y_relay(dist, True, i).start()

        slot = 4 - dist

        @pl.when(jnp.logical_not(from_below(slot)))
        def _():
            landed(raw.at[slot, part(i)], y_recv.at[slot, i])
            if dist < 4:
                y_relay(slot, False, i).start()

    def z_event(k, i):
        if k < 4:
            landed(raw.at[UP[k], part(i)], z_recv.at[UP[k] - 5, i])
            if k < 3:
                z_relay(UP[k], UP[k + 1], i, True).start()
            else:
                @pl.when(i < NCH // 2)
                def _():
                    z_relay(UP[3], UP[4], i, True).start()
            landed(raw.at[DOWN[k], part(i)], z_recv.at[DOWN[k] - 5, i])
            if k < 3:
                z_relay(DOWN[k], DOWN[k + 1], i, False).start()
            else:
                @pl.when(i >= NCH // 2)
                def _():
                    z_relay(DOWN[3], UP[4], i, False).start()
        else:
            landed(raw.at[UP[4], part(i)], z_recv.at[UP[4] - 5, i])

    def each(body):
        lax.fori_loop(0, NCH, lambda i, _: (body(i), 0)[1], 0)

    @pl.when(first)
    def _():
        def go(i):
            y_own_up(i).start()
            z_start(x_ref, i, True).start()
            z_start(x_ref, i, False).start()
        each(go)

    @pl.when(other)
    def _():
        def go(i):
            y_own_down(i).start()
            y_own_partner(i).start()
        each(go)

    sums = jnp.sum(x_ref[...], axis=0, keepdims=True)
    zs[z] = jnp.zeros((8, LANES), jnp.float32)
    for k in range(COLS):
        zs[z, k : k + 1, :] = sums[:, k * LANES : (k + 1) * LANES]

    def ms_copy(k):
        return remote(zs.at[z], zs.at[z], ms_send.at[k - 1], ms_recv.at[k - 1], at_z(k))

    for k in range(1, 8):
        ms_copy(k).start()

    def phase_one(dist):
        def step(i):
            y_event(dist, i)

            @pl.when(first)
            def _():
                z_event(dist, i)

            if dist == 4:
                @pl.when(other)
                def _():
                    z_start(raw.at[0], i, True).start()
                    z_start(raw.at[0], i, False).start()
        each(step)

    phase_one(1)

    mine = 2 * a + c

    def mt_copy(k):
        return remote(zt, ys.at[mine], mt_send.at[k], mt_recv.at[mine], at_y(k, h))

    for k in range(1, 8):
        source = rem(z + 8 - k, 8)
        landed(zs.at[source], ms_recv.at[k - 1])
    total = zs[0]
    for k in range(1, 8):
        total = total + zs[k]
    zt[...] = total
    for k in range(1, 8):
        mt_copy(k).start()

    @pl.when(first)
    def _():
        ys[mine] = total

    @pl.when(other)
    def _():
        mt_copy(0).start()

    for dist in range(2, 5):
        phase_one(dist)

    @pl.when(first)
    def _():
        each(lambda i: landed(raw.at[4, part(i)], y_recv.at[4, i]))
        raw[0] = x_ref[...]

    for k in range(8):
        @pl.when(jnp.logical_or(other, mine != k))
        def _():
            landed(ys.at[k], mt_recv.at[k])
    total = ys[0]
    for k in range(1, 8):
        total = total + ys[k]
    mean[...] = total * (1.0 / NSAMPLES)

    def convert(slot):
        m = mean[...]
        row = jnp.concatenate([m[k : k + 1, :] for k in range(COLS)], axis=1)
        value = raw[slot] - row
        top = value.astype(jnp.bfloat16)
        hi[slot] = top
        lo[slot] = (value - top.astype(jnp.float32)).astype(jnp.bfloat16)

    lax.fori_loop(0, 5, lambda s, _: (convert(s), 0)[1], 0)

    e_mine = y

    def pair(r, j):
        e_low = rem(e_mine + 8 - r, 8)
        low = 16 * rem(e_low, 4) + 2 * z + div(e_low, 4)
        z_high = rem(z + 8 + j, 8)
        high = 16 * a + 2 * z_high + h
        gap = rem(high + NB - low, NB)
        keep = gap <= HALF
        a_row = jnp.where(keep, rem(e_low, 4), a)
        z_row = jnp.where(keep, z, z_high)
        c_row = jnp.where(keep, div(e_low, 4), h)
        d = jnp.where(keep, gap, NB - gap)
        return keep, gap, (a_row, z_row, c_row), d

    def slot_of(j):
        return jnp.where(j >= 0, jnp.where(j == 0, 0, 4 + j), 8 - j)

    def tile_of(k, t):
        if k == 0:
            return jnp.where(t == 5, 2, t), jnp.int32(0) * t, t == 5
        if k == 4:
            return t, 4 + jnp.int32(0) * t, t < 0
        return jnp.where(t < 5, t, t - 4), jnp.where(t < 5, k, -k), t < 0

    contract = (((1,), (1,)), ((), ()))

    def dot(p, q):
        return lax.dot_general(p, q, contract, preferred_element_type=jnp.float32)

    def compute(k, t):
        r, j, swap = tile_of(k, t)
        keep, _, _, _ = pair(r, j)
        keep = jnp.logical_xor(keep, swap)
        row = jnp.where(keep, r, slot_of(j))
        col = jnp.where(keep, slot_of(j), r)
        acc = dot(hi[row], hi[col]) + dot(hi[row], lo[col]) + dot(lo[row], hi[col])
        index = GROUPS[k][0] + t
        for xx in range(4):
            for yy in range(2):
                start = 32 * xx + 16 * yy
                pk[yy, xx, index] = acc[start : start + 16, :]

    def d_copy(k):
        t0, n = GROUPS[k]
        return remote(
            pk.at[1 - c, :, pl.ds(t0, n)], pr.at[:, pl.ds(t0, n)], d_send.at[k], d_recv.at[k], partner
        )

    def x_copy(k, s):
        t0, n = GROUPS[k]
        return remote(
            sx.at[rem(x + s, 4), pl.ds(t0, n)], xr.at[s - 1, pl.ds(t0, n)],
            x_send.at[k, s - 1], x_recv.at[k, s - 1], at_x(s),
        )

    def over_cores(k):
        t0, n = GROUPS[k]
        landed(pr.at[:, pl.ds(t0, n)], d_recv.at[k])
        sx[:, t0 : t0 + n] = pk[c, :, t0 : t0 + n] + pr[:, t0 : t0 + n]
        for s in range(1, 4):
            x_copy(k, s).start()

    def target(k, t):
        r, j, swap = tile_of(k, t)
        keep, gap, (a_row, z_row, c_row), d = pair(r, j)
        valid = jnp.logical_not(jnp.logical_and(swap, gap != HALF))
        low = jnp.logical_and(r == 0, j == 4)
        valid = jnp.logical_and(valid, jnp.logical_or(jnp.logical_not(low), z < 4))
        low = jnp.logical_and(r == 4, j == 0)
        valid = jnp.logical_and(valid, jnp.logical_or(jnp.logical_not(low), h == 0))
        low = jnp.logical_and(r == 4, j == 4)
        valid = jnp.logical_and(valid, jnp.logical_or(jnp.logical_not(low), h == 1))
        a_row = jnp.where(swap, a, a_row)
        z_row = jnp.where(swap, z, z_row)
        c_row = jnp.where(swap, h, c_row)
        local = (a_row == a) & (z_row == z) & (c_row == c) & (c == h)
        return valid, local, (a_row, z_row, c_row, x, c), d

    def f_copy(k, t):
        _, _, device, d = target(k, t)
        index = GROUPS[k][0] + t
        return remote(fb.at[index], out_ref.at[0, d], f_send.at[index], f_recv.at[d], device)

    def over_planes(k):
        t0, n = GROUPS[k]
        for s in range(1, 4):
            landed(xr.at[s - 1, pl.ds(t0, n)], x_recv.at[k, s - 1])
        block = pl.ds(t0, n)
        fb[block] = (sx[x, block] + xr[0, block] + xr[1, block] + xr[2, block]) * (1.0 / NPARAMS)

        def send(t, carry):
            valid, local, _, d = target(k, t)

            @pl.when(jnp.logical_and(valid, local))
            def _():
                out_ref[0, d] = fb[t0 + t]

            @pl.when(jnp.logical_and(valid, jnp.logical_not(local)))
            def _():
                f_copy(k, t).start()

            return carry

        lax.fori_loop(0, n, send, 0)

    for k in range(5):
        if 1 <= k <= 3:
            convert(UP[k])
            convert(DOWN[k])
        if k == 4:
            convert(UP[4])
        n = GROUPS[k][1]
        per = -(-n // NCH)

        def step(i):
            if k < 4:
                @pl.when(other)
                def _():
                    z_event(k + 1, i)
            for u in range(per):
                if per * NCH <= n:
                    compute(k, i * per + u)
                else:
                    @pl.when(i * per + u < n)
                    def _():
                        compute(k, i * per + u)

        each(step)
        d_copy(k).start()
        over_cores(k)
        if k:
            over_planes(k - 1)
    over_planes(4)

    def arrived(d, carry):
        step = div(d, 2)
        local = (rem(d, 2) == 0) & (step <= 4) & (z + step <= 7)
        for r in range(1, 5):
            _, gap, _, _ = pair(r, 0)
            here = (gap >= HALF) & (d == NB - gap)
            local = local | ((here & (h == 0)) if r == 4 else here)
        local = local & first

        @pl.when(jnp.logical_not(local))
        def _():
            landed(out_ref.at[0, d], f_recv.at[d])

        return carry

    lax.fori_loop(0, HALF + 1, arrived, 0)

    def sent(i):
        @pl.when(first)
        def _():
            y_own_up(i).wait_send()

        @pl.when(other)
        def _():
            y_own_down(i).wait_send()
            y_own_partner(i).wait_send()

        z_start(x_ref, i, True).wait_send()
        z_start(x_ref, i, False).wait_send()
        for dist in range(1, 4):
            @pl.when(from_below(dist))
            def _():
                y_relay(dist, True, i).wait_send()

            @pl.when(jnp.logical_not(from_below(4 - dist)))
            def _():
                y_relay(4 - dist, False, i).wait_send()
        for k in range(1, 3):
            z_relay(UP[k], UP[k + 1], i, True).wait_send()
            z_relay(DOWN[k], DOWN[k + 1], i, False).wait_send()

        @pl.when(i < NCH // 2)
        def _():
            z_relay(UP[3], UP[4], i, True).wait_send()

        @pl.when(i >= NCH // 2)
        def _():
            z_relay(DOWN[3], UP[4], i, False).wait_send()

    each(sent)
    for k in range(1, 8):
        ms_copy(k).wait_send()
        mt_copy(k).wait_send()

    @pl.when(other)
    def _():
        mt_copy(0).wait_send()

    for k in range(5):
        d_copy(k).wait_send()
        for s in range(1, 4):
            x_copy(k, s).wait_send()

        def gone(t, carry):
            valid, local, _, _ = target(k, t)

            @pl.when(jnp.logical_and(valid, jnp.logical_not(local)))
            def _():
                f_copy(k, t).wait_send()

            return carry

        lax.fori_loop(0, GROUPS[k][1], gone, 0)


def on_device(logder):
    f32, bf16 = jnp.float32, jnp.bfloat16
    dma = pltpu.SemaphoreType.DMA
    return pl.pallas_call(
        kernel,
        out_shape=jax.ShapeDtypeStruct((1, HALF + 1, 16, ROWS), f32),
        in_specs=[pl.BlockSpec(memory_space=pltpu.VMEM)],
        out_specs=pl.BlockSpec(memory_space=pltpu.VMEM),
        scratch_shapes=[
            pltpu.VMEM((NSLOT, ROWS, WIDTH), f32),
            pltpu.VMEM((NSLOT, ROWS, WIDTH), bf16),
            pltpu.VMEM((NSLOT, ROWS, WIDTH), bf16),
            pltpu.VMEM((8, 8, LANES), f32),
            pltpu.VMEM((8, LANES), f32),
            pltpu.VMEM((8, 8, LANES), f32),
            pltpu.VMEM((8, LANES), f32),
            pltpu.VMEM((2, 4, NTILE, 16, ROWS), f32),
            pltpu.VMEM((4, NTILE, 16, ROWS), f32),
            pltpu.VMEM((4, NTILE, 16, ROWS), f32),
            pltpu.VMEM((3, NTILE, 16, ROWS), f32),
            pltpu.VMEM((NTILE, 16, ROWS), f32),
            dma((2, NCH)),
            dma((5, NCH)),
            dma((5, NCH)),
            dma((7, NCH)),
            dma((2, NCH)),
            dma((7, NCH)),
            dma((7,)),
            dma((7,)),
            dma((8,)),
            dma((8,)),
            dma((5,)),
            dma((5,)),
            dma((5, 3)),
            dma((5, 3)),
            dma((NTILE,)),
            dma((HALF + 1,)),
        ],
        compiler_params=pltpu.CompilerParams(collective_id=0, has_side_effects=True),
    )(logder)


def solution(mesh):
    torus = Mesh(mesh.devices.reshape(4, 8, 2, 4, 2), ("a", "z", "c", "x", "h"))
    return jax.shard_map(
        on_device,
        mesh=torus,
        in_specs=(P(("a", "z", "c"), ("x", "h")),),
        out_specs=P(("a", "z", "c"), None, ("x", "h"), None),
        check_vma=False,
    )
```

```python
import jax
import jax.numpy as jnp
from jax import lax
from jax.experimental import pallas as pl
from jax.experimental.pallas import tpu as pltpu
from jax.sharding import Mesh
from jax.sharding import PartitionSpec as P

MESH = pl.DeviceIdType.MESH

ROWS, WIDTH = 128, 768
LANES = 128
COLS = WIDTH // LANES
NCH = 4
CH = ROWS // NCH
NB = 64
HALF = 32
NSAMPLES = 8192
SUMS_AT = 2
NPARAMS = 6144

NSLOT = 12
UP = {1: 5, 2: 6, 3: 7, 4: 8}
DOWN = {1: 9, 2: 10, 3: 11}

GROUPS = [(0, 6), (6, 8), (14, 8), (22, 8), (30, 5)]
NTILE = 35


def rem(value, count):
    return lax.rem(value, jnp.int32(count))


def div(value, count):
    return lax.div(value, jnp.int32(count))


def kernel(
    x_ref, out_ref, raw, hi, lo, zs, zt, ys, mean, pk, pr, xr, fb, home,
    own_send, y_send, y_recv, z_send, z_own, z_recv, ms_send, ms_recv, mt_send, mt_recv,
    known, d_send, d_recv, x_send, x_recv, f_send, f_recv, g_send, g_recv,
):
    a = lax.axis_index("a")
    z = lax.axis_index("z")
    c = lax.axis_index("c")
    x = lax.axis_index("x")
    h = lax.axis_index("h")
    y = h * 4 + a
    first = c == h
    other = c != h

    def at_y(steps, core):
        yy = rem(y + 8 + steps, 8)
        return (rem(yy, 4), z, core, x, div(yy, 4))

    def at_z(steps):
        return (a, rem(z + 8 + steps, 8), c, x, h)

    def at_x(steps):
        return (a, z, c, rem(x + steps, 4), h)

    partner = (a, z, 1 - c, x, h)

    def remote(src, dst, send, recv, device):
        return pltpu.make_async_remote_copy(
            src_ref=src, dst_ref=dst, send_sem=send, recv_sem=recv,
            device_id=device, device_id_type=MESH,
        )

    def landed(ref, sem):
        pltpu.make_async_copy(ref, ref, sem).wait()

    barrier = pltpu.get_barrier_semaphore()

    def hello(device):
        pl.semaphore_signal(barrier, inc=1, device_id=device, device_id_type=MESH)

    hello(partner)
    for k in (1, 7):
        hello(at_z(k))
        hello(at_y(k, 0))
        hello(at_y(k, 1))
    for k in range(1, 4):
        hello(at_x(k))
    pl.semaphore_wait(barrier, 10)

    def spread(turn):
        if turn > 0:
            for way in range(4):
                pl.semaphore_wait(known.at[way], 1)
        if turn < 3:
            for way, device in enumerate((at_z(1), at_z(-1), at_y(1, c), at_y(-1, c))):
                pl.semaphore_signal(known.at[way], inc=1, device_id=device, device_id_type=MESH)

    def part(i):
        return pl.ds(pl.multiple_of(i * CH, CH), CH)

    def from_below(r):
        return div(rem(y + 8 - r, 8), 4) == c

    def y_own_up(i):
        return remote(x_ref.at[part(i)], raw.at[1, part(i)], own_send.at[0, i], y_recv.at[1, i], at_y(1, c))

    def y_own_down(i):
        return remote(
            x_ref.at[part(i)], raw.at[3, part(i)], own_send.at[0, i], y_recv.at[3, i], at_y(-1, 1 - c)
        )

    def y_own_partner(i):
        return remote(x_ref.at[part(i)], raw.at[4, part(i)], own_send.at[1, i], y_recv.at[4, i], partner)

    def y_relay(r, up, i):
        to = r + 1 if up else r - 1
        return remote(
            raw.at[r, part(i)], raw.at[to, part(i)], y_send.at[r, i], y_recv.at[to, i],
            at_y(1 if up else -1, c),
        )

    def z_start(src, i, low):
        to = UP[1] if low else DOWN[1]
        return remote(
            src.at[part(i)], raw.at[to, part(i)], z_own.at[0 if low else 1, i], z_recv.at[to - 5, i],
            at_z(-1 if low else 1),
        )

    def z_relay(slot, to, i, low):
        return remote(
            raw.at[slot, part(i)], raw.at[to, part(i)], z_send.at[slot - 5, i], z_recv.at[to - 5, i],
            at_z(-1 if low else 1),
        )

    def y_event(dist, i):
        @pl.when(from_below(dist))
        def _():
            landed(raw.at[dist, part(i)], y_recv.at[dist, i])
            if dist < 4:
                y_relay(dist, True, i).start()

        slot = 4 - dist

        @pl.when(jnp.logical_not(from_below(slot)))
        def _():
            landed(raw.at[slot, part(i)], y_recv.at[slot, i])
            if dist < 4:
                y_relay(slot, False, i).start()

    def z_event(k, i):
        if k < 4:
            landed(raw.at[UP[k], part(i)], z_recv.at[UP[k] - 5, i])
            if k < 3:
                z_relay(UP[k], UP[k + 1], i, True).start()
            else:
                if i < NCH // 2:
                    z_relay(UP[3], UP[4], i, True).start()
            landed(raw.at[DOWN[k], part(i)], z_recv.at[DOWN[k] - 5, i])
            if k < 3:
                z_relay(DOWN[k], DOWN[k + 1], i, False).start()
            elif i >= NCH // 2:
                z_relay(DOWN[3], UP[4], i, False).start()
        else:
            landed(raw.at[UP[4], part(i)], z_recv.at[UP[4] - 5, i])

    def each(body):
        lax.fori_loop(0, NCH, lambda i, _: (body(i), 0)[1], 0)

    @pl.when(first)
    def _():
        def go(i):
            y_own_up(i).start()
            z_start(x_ref, i, True).start()
            z_start(x_ref, i, False).start()
        each(go)

    @pl.when(other)
    def _():
        def go(i):
            y_own_down(i).start()
            y_own_partner(i).start()
        each(go)

    spread(0)

    sums = jnp.sum(x_ref[...], axis=0, keepdims=True)
    zs[z] = jnp.zeros((8, LANES), jnp.float32)
    for k in range(COLS):
        zs[z, k : k + 1, :] = sums[:, k * LANES : (k + 1) * LANES]

    def ms_copy(k):
        return remote(zs.at[z], zs.at[z], ms_send.at[k - 1], ms_recv.at[k - 1], at_z(k))

    mine = 2 * a + c

    def mt_copy(k):
        return remote(zt, ys.at[mine], mt_send.at[k], mt_recv.at[mine], at_y(k, h))

    def sums_over_z():
        for k in range(1, 8):
            source = rem(z + 8 - k, 8)
            landed(zs.at[source], ms_recv.at[k - 1])
        total = zs[0]
        for k in range(1, 8):
            total = total + zs[k]
        zt[...] = total
        for k in range(1, 8):
            mt_copy(k).start()

        @pl.when(first)
        def _():
            ys[mine] = total

        @pl.when(other)
        def _():
            mt_copy(0).start()

    for k in range(1, 5):
        for i in range(NCH):
            y_event(k, i)

            @pl.when(first)
            def _():
                z_event(k, i)

            if k == 4:
                @pl.when(other)
                def _():
                    z_start(raw.at[0], i, True).start()
                    z_start(raw.at[0], i, False).start()
            if k == 1 and i < 3:
                spread(i + 1)
            if k == 1 and i == 2:
                for j in range(1, 8):
                    ms_copy(j).start()
        if k == SUMS_AT:
            sums_over_z()

    @pl.when(first)
    def _():
        each(lambda i: landed(raw.at[4, part(i)], y_recv.at[4, i]))
        raw[0] = x_ref[...]

    for k in range(8):
        @pl.when(jnp.logical_or(other, mine != k))
        def _():
            landed(ys.at[k], mt_recv.at[k])
    total = ys[0]
    for k in range(1, 8):
        total = total + ys[k]
    mean[...] = total * (1.0 / NSAMPLES)

    def convert(slot):
        m = mean[...]
        row = jnp.concatenate([m[k : k + 1, :] for k in range(COLS)], axis=1)
        value = raw[slot] - row
        top = value.astype(jnp.bfloat16)
        hi[slot] = top
        lo[slot] = (value - top.astype(jnp.float32)).astype(jnp.bfloat16)

    e_mine = y

    def pair(r, j):
        e_low = rem(e_mine + 8 - r, 8)
        low = 16 * rem(e_low, 4) + 2 * z + div(e_low, 4)
        z_high = rem(z + 8 + j, 8)
        high = 16 * a + 2 * z_high + h
        gap = rem(high + NB - low, NB)
        keep = gap <= HALF
        a_row = jnp.where(keep, rem(e_low, 4), a)
        z_row = jnp.where(keep, z, z_high)
        c_row = jnp.where(keep, div(e_low, 4), h)
        d = jnp.where(keep, gap, NB - gap)
        return keep, gap, (a_row, z_row, c_row), d

    def slot_of(j):
        return jnp.where(j >= 0, jnp.where(j == 0, 0, 4 + j), 8 - j)

    def tile_of(k, t):
        if k == 0:
            return jnp.where(t == 5, 2, t), jnp.int32(0) * t, t == 5
        if k == 4:
            return t, 4 + jnp.int32(0) * t, t < 0
        return jnp.where(t < 5, t, t - 4), jnp.where(t < 5, k, -k), t < 0

    contract = (((1,), (1,)), ((), ()))

    def dot(p, q):
        return lax.dot_general(p, q, contract, preferred_element_type=jnp.float32)

    def compute(k, t):
        r, j, swap = tile_of(k, t)
        keep, _, _, _ = pair(r, j)
        keep = jnp.logical_xor(keep, swap)
        row = jnp.where(keep, r, slot_of(j))
        col = jnp.where(keep, slot_of(j), r)
        acc = dot(hi[row], hi[col]) + dot(hi[row], lo[col]) + dot(lo[row], hi[col])
        index = GROUPS[k][0] + t
        for xx in range(4):
            for yy in range(2):
                start = 32 * xx + 16 * yy
                pk[xx, index, yy] = acc[start : start + 16, :]

    def d_copy(k):
        t0, n = GROUPS[k]
        tiles = pl.ds(t0, n)
        return remote(pk.at[:, tiles], pr.at[:, tiles], d_send.at[k], d_recv.at[k], partner)

    def x_copy(k, s):
        t0, n = GROUPS[k]
        return remote(
            pk.at[rem(x + s, 4), pl.ds(t0, n)], xr.at[s - 1, pl.ds(t0, n)],
            x_send.at[k, s - 1], x_recv.at[k, s - 1], at_x(s),
        )

    def over_cores(k):
        t0, n = GROUPS[k]
        tiles = pl.ds(t0, n)
        landed(pr.at[:, tiles], d_recv.at[k])
        pk[:, tiles] = pk[:, tiles] + pr[:, tiles]

    def target(k, t):
        r, j, swap = tile_of(k, t)
        keep, gap, (a_row, z_row, c_row), d = pair(r, j)
        valid = jnp.logical_not(jnp.logical_and(swap, gap != HALF))
        low = jnp.logical_and(r == 0, j == 4)
        valid = jnp.logical_and(valid, jnp.logical_or(jnp.logical_not(low), z < 4))
        low = jnp.logical_and(r == 4, j == 0)
        valid = jnp.logical_and(valid, jnp.logical_or(jnp.logical_not(low), h == 0))
        low = jnp.logical_and(r == 4, j == 4)
        valid = jnp.logical_and(valid, jnp.logical_or(jnp.logical_not(low), h == 1))
        a_row = jnp.where(swap, a, a_row)
        z_row = jnp.where(swap, z, z_row)
        c_row = jnp.where(swap, h, c_row)
        mine = (a_row == a) & (z_row == z) & (c_row == c)
        return valid, mine, (a_row, z_row, c_row), d

    def f_copy(k, t, row, d, hh):
        index = GROUPS[k][0] + t
        return remote(
            fb.at[index, hh], out_ref.at[0, d], f_send.at[index, hh], f_recv.at[d], (*row, x, hh)
        )

    def g_copy(t, row, d, xx, hh):
        return remote(
            pk.at[xx, GROUPS[4][0] + t, hh], home.at[x, d],
            g_send.at[t, xx, hh], g_recv.at[x, d], (*row, xx, hh),
        )

    def over_planes(k):
        t0, n = GROUPS[k]
        for s in range(1, 4):
            landed(xr.at[s - 1, pl.ds(t0, n)], x_recv.at[k, s - 1])
        tiles = pl.ds(t0, n)
        fb[tiles] = (pk[x, tiles] + xr[0, tiles] + xr[1, tiles] + xr[2, tiles]) * (1.0 / NPARAMS)

        def send(t, carry):
            valid, mine, row, d = target(k, t)
            for hh in range(2):
                local = mine & (h == hh)

                @pl.when(jnp.logical_and(valid, local))
                def _():
                    out_ref[0, d] = fb[t0 + t, hh]

                @pl.when(jnp.logical_and(valid, jnp.logical_not(local)))
                def _():
                    f_copy(k, t, row, d, hh).start()

            return carry

        lax.fori_loop(0, n, send, 0)

    def go_home():
        def send(t, carry):
            valid, mine, row, d = target(4, t)
            for xx in range(4):
                for hh in range(2):
                    local = mine & (h == hh) & (x == xx)

                    @pl.when(jnp.logical_and(valid, local))
                    def _():
                        home[xx, d] = pk[xx, GROUPS[4][0] + t, hh]

                    @pl.when(jnp.logical_and(valid, jnp.logical_not(local)))
                    def _():
                        g_copy(t, row, d, xx, hh).start()

            return carry

        lax.fori_loop(0, GROUPS[4][1], send, 0)

    def some(k, start, stop):
        lax.fori_loop(start, stop, lambda t, _: (compute(k, t), 0)[1], 0)

    def arrives(k, i):
        @pl.when(other)
        def _():
            z_event(k, i)

    for k in range(5):
        n = GROUPS[k][1]
        if k < 4:
            arrives(k + 1, 0)
        if k == 0:
            lax.fori_loop(0, 5, lambda s, _: (convert(s), 0)[1], 0)
        elif k < 4:
            convert(UP[k])
            convert(DOWN[k])
        else:
            convert(UP[4])
        some(k, 0, n // 2)
        if k < 4:
            arrives(k + 1, 1)
        some(k, n // 2, n)

        @pl.when(first)
        def _():
            d_copy(k).start()

        @pl.when(other)
        def _():
            if k < 4:
                z_event(k + 1, 2)
            over_cores(k)
            if k < 4:
                for s in range(1, 4):
                    x_copy(k, s).start()
                z_event(k + 1, 3)
            else:
                go_home()
            if k:
                over_planes(k - 1)

    def arrived(d, carry):
        local = d < 0
        for j in range(5):
            gap = rem(2 * (rem(z + j, 8) - z) + h - c + NB, NB)
            here = d == gap
            if j == 0:
                here = here & (h == 0)
            if j == 4:
                here = here & (h == 1)
            local = local | here
        local = local & other
        last = rem(div(rem(16 * a + 2 * z + c + d, NB), 2) + 8 - z, 8) == 4

        @pl.when(last)
        def _():
            for xx in range(4):
                @pl.when(jnp.logical_not(local & (x == xx)))
                def _():
                    landed(home.at[xx, d], g_recv.at[xx, d])
            out_ref[0, d] = (home[0, d] + home[1, d] + home[2, d] + home[3, d]) * (1.0 / NPARAMS)

        @pl.when(jnp.logical_not(last | local))
        def _():
            landed(out_ref.at[0, d], f_recv.at[d])

        return carry

    lax.fori_loop(0, HALF + 1, arrived, 0)

    def sent(i):
        @pl.when(first)
        def _():
            y_own_up(i).wait_send()

        @pl.when(other)
        def _():
            y_own_down(i).wait_send()
            y_own_partner(i).wait_send()

        z_start(x_ref, i, True).wait_send()
        z_start(x_ref, i, False).wait_send()
        for dist in range(1, 4):
            @pl.when(from_below(dist))
            def _():
                y_relay(dist, True, i).wait_send()

            @pl.when(jnp.logical_not(from_below(4 - dist)))
            def _():
                y_relay(4 - dist, False, i).wait_send()
        for k in range(1, 3):
            z_relay(UP[k], UP[k + 1], i, True).wait_send()
            z_relay(DOWN[k], DOWN[k + 1], i, False).wait_send()

        @pl.when(i < NCH // 2)
        def _():
            z_relay(UP[3], UP[4], i, True).wait_send()

        @pl.when(i >= NCH // 2)
        def _():
            z_relay(DOWN[3], UP[4], i, False).wait_send()

    each(sent)
    for k in range(1, 8):
        ms_copy(k).wait_send()
        mt_copy(k).wait_send()

    @pl.when(first)
    def _():
        for k in range(5):
            d_copy(k).wait_send()

    @pl.when(other)
    def _():
        mt_copy(0).wait_send()
        for k in range(4):
            for s in range(1, 4):
                x_copy(k, s).wait_send()

            def gone(t, carry):
                valid, mine, row, d = target(k, t)
                for hh in range(2):
                    @pl.when(jnp.logical_and(valid, jnp.logical_not(mine & (h == hh))))
                    def _():
                        f_copy(k, t, row, d, hh).wait_send()
                return carry

            lax.fori_loop(0, GROUPS[k][1], gone, 0)

        def left(t, carry):
            valid, mine, row, d = target(4, t)
            for xx in range(4):
                for hh in range(2):
                    @pl.when(jnp.logical_and(valid, jnp.logical_not(mine & (h == hh) & (x == xx))))
                    def _():
                        g_copy(t, row, d, xx, hh).wait_send()
            return carry

        lax.fori_loop(0, GROUPS[4][1], left, 0)


def on_device(logder):
    f32, bf16 = jnp.float32, jnp.bfloat16
    dma = pltpu.SemaphoreType.DMA
    return pl.pallas_call(
        kernel,
        out_shape=jax.ShapeDtypeStruct((1, HALF + 1, 16, ROWS), f32),
        in_specs=[pl.BlockSpec(memory_space=pltpu.VMEM)],
        out_specs=pl.BlockSpec(memory_space=pltpu.VMEM),
        scratch_shapes=[
            pltpu.VMEM((NSLOT, ROWS, WIDTH), f32),
            pltpu.VMEM((NSLOT, ROWS, WIDTH), bf16),
            pltpu.VMEM((NSLOT, ROWS, WIDTH), bf16),
            pltpu.VMEM((8, 8, LANES), f32),
            pltpu.VMEM((8, LANES), f32),
            pltpu.VMEM((8, 8, LANES), f32),
            pltpu.VMEM((8, LANES), f32),
            pltpu.VMEM((4, NTILE, 2, 16, ROWS), f32),
            pltpu.VMEM((4, NTILE, 2, 16, ROWS), f32),
            pltpu.VMEM((3, NTILE, 2, 16, ROWS), f32),
            pltpu.VMEM((NTILE, 2, 16, ROWS), f32),
            pltpu.VMEM((4, HALF + 1, 16, ROWS), f32),
            dma((2, NCH)),
            dma((5, NCH)),
            dma((5, NCH)),
            dma((7, NCH)),
            dma((2, NCH)),
            dma((7, NCH)),
            dma((7,)),
            dma((7,)),
            dma((8,)),
            dma((8,)),
            pltpu.SemaphoreType.REGULAR((4,)),
            dma((5,)),
            dma((5,)),
            dma((5, 3)),
            dma((5, 3)),
            dma((NTILE, 2)),
            dma((HALF + 1,)),
            dma((5, 4, 2)),
            dma((4, HALF + 1)),
        ],
        compiler_params=pltpu.CompilerParams(collective_id=0, has_side_effects=True),
    )(logder)


def solution(mesh):
    torus = Mesh(mesh.devices.reshape(4, 8, 2, 4, 2), ("a", "z", "c", "x", "h"))
    return jax.shard_map(
        on_device,
        mesh=torus,
        in_specs=(P(("a", "z", "c"), ("x", "h")),),
        out_specs=P(("a", "z", "c"), None, ("x", "h"), None),
        check_vma=False,
    )
```

```python
import jax
import jax.numpy as jnp
from jax import lax
from jax.experimental import pallas as pl
from jax.experimental.pallas import tpu as pltpu
from jax.sharding import Mesh
from jax.sharding import PartitionSpec as P

MESH = pl.DeviceIdType.MESH

ROWS, WIDTH = 128, 768
LANES = 128
COLS = WIDTH // LANES
NCH = 4
CH = ROWS // NCH
NB = 64
HALF = 32
NSAMPLES = 8192
SUMS_AT = 2
NPARAMS = 6144

NSLOT = 12
UP = {1: 5, 2: 6, 3: 7, 4: 8}
DOWN = {1: 9, 2: 10, 3: 11}

GROUPS = [(0, 6), (6, 8), (14, 8), (22, 8), (30, 5)]
NTILE = 35


def rem(value, count):
    return lax.rem(value, jnp.int32(count))


def div(value, count):
    return lax.div(value, jnp.int32(count))


def kernel(
    x_ref, out_ref, raw, hl, zs, zt, ys, mean, pk, pr, xr, fb, home,
    own_send, y_send, y_recv, z_send, z_own, z_recv, ms_send, ms_recv, mt_send, mt_recv,
    known, d_send, d_recv, x_send, x_recv, f_send, f_recv, g_send, g_recv,
):
    a = lax.axis_index("a")
    z = lax.axis_index("z")
    c = lax.axis_index("c")
    x = lax.axis_index("x")
    h = lax.axis_index("h")
    y = h * 4 + a
    first = c == h
    other = c != h

    def at_y(steps, core):
        yy = rem(y + 8 + steps, 8)
        return (rem(yy, 4), z, core, x, div(yy, 4))

    def at_z(steps):
        return (a, rem(z + 8 + steps, 8), c, x, h)

    def at_x(steps):
        return (a, z, c, rem(x + steps, 4), h)

    partner = (a, z, 1 - c, x, h)

    def remote(src, dst, send, recv, device):
        return pltpu.make_async_remote_copy(
            src_ref=src, dst_ref=dst, send_sem=send, recv_sem=recv,
            device_id=device, device_id_type=MESH,
        )

    def landed(ref, sem):
        pltpu.make_async_copy(ref, ref, sem).wait()

    barrier = pltpu.get_barrier_semaphore()

    def hello(device):
        pl.semaphore_signal(barrier, inc=1, device_id=device, device_id_type=MESH)

    hello(partner)
    for k in (1, 7):
        hello(at_z(k))
        hello(at_y(k, 0))
        hello(at_y(k, 1))
    for k in range(1, 4):
        hello(at_x(k))
    pl.semaphore_wait(barrier, 10)

    def spread(turn):
        if turn > 0:
            for way in range(4):
                pl.semaphore_wait(known.at[way], 1)
        if turn < 3:
            for way, device in enumerate((at_z(1), at_z(-1), at_y(1, c), at_y(-1, c))):
                pl.semaphore_signal(known.at[way], inc=1, device_id=device, device_id_type=MESH)

    def part(i):
        return pl.ds(pl.multiple_of(i * CH, CH), CH)

    def from_below(r):
        return div(rem(y + 8 - r, 8), 4) == c

    def y_own_up(i):
        return remote(x_ref.at[part(i)], raw.at[1, part(i)], own_send.at[0], y_recv.at[1, i], at_y(1, c))

    def y_own_down(i):
        return remote(
            x_ref.at[part(i)], raw.at[3, part(i)], own_send.at[0], y_recv.at[3, i], at_y(-1, 1 - c)
        )

    def y_own_partner(i):
        return remote(x_ref.at[part(i)], raw.at[4, part(i)], own_send.at[1], y_recv.at[4, i], partner)

    def y_relay(r, up, i):
        to = r + 1 if up else r - 1
        return remote(
            raw.at[r, part(i)], raw.at[to, part(i)], y_send.at[r], y_recv.at[to, i],
            at_y(1 if up else -1, c),
        )

    def z_start(src, i, low):
        to = UP[1] if low else DOWN[1]
        return remote(
            src.at[part(i)], raw.at[to, part(i)], z_own.at[0 if low else 1], z_recv.at[to - 5, i],
            at_z(-1 if low else 1),
        )

    def z_relay(slot, to, i, low):
        return remote(
            raw.at[slot, part(i)], raw.at[to, part(i)], z_send.at[slot - 5], z_recv.at[to - 5, i],
            at_z(-1 if low else 1),
        )

    def y_event(dist, i):
        @pl.when(from_below(dist))
        def _():
            landed(raw.at[dist, part(i)], y_recv.at[dist, i])
            if dist < 4:
                y_relay(dist, True, i).start()

        slot = 4 - dist

        @pl.when(jnp.logical_not(from_below(slot)))
        def _():
            landed(raw.at[slot, part(i)], y_recv.at[slot, i])
            if dist < 4:
                y_relay(slot, False, i).start()

    def z_event(k, i):
        if k < 4:
            landed(raw.at[UP[k], part(i)], z_recv.at[UP[k] - 5, i])
            if k < 3:
                z_relay(UP[k], UP[k + 1], i, True).start()
            else:
                if i < NCH // 2:
                    z_relay(UP[3], UP[4], i, True).start()
            landed(raw.at[DOWN[k], part(i)], z_recv.at[DOWN[k] - 5, i])
            if k < 3:
                z_relay(DOWN[k], DOWN[k + 1], i, False).start()
            elif i >= NCH // 2:
                z_relay(DOWN[3], UP[4], i, False).start()
        else:
            landed(raw.at[UP[4], part(i)], z_recv.at[UP[4] - 5, i])

    def each(body):
        lax.fori_loop(0, NCH, lambda i, _: (body(i), 0)[1], 0)

    @pl.when(first)
    def _():
        def go(i):
            y_own_up(i).start()
            z_start(x_ref, i, True).start()
            z_start(x_ref, i, False).start()
        each(go)

    @pl.when(other)
    def _():
        def go(i):
            y_own_down(i).start()
            y_own_partner(i).start()
        each(go)

    spread(0)

    sums = jnp.sum(x_ref[...], axis=0, keepdims=True)
    zs[z] = jnp.zeros((8, LANES), jnp.float32)
    for k in range(COLS):
        zs[z, k : k + 1, :] = sums[:, k * LANES : (k + 1) * LANES]

    def ms_copy(k):
        return remote(zs.at[z], zs.at[z], ms_send, ms_recv, at_z(k))

    mine = 2 * a + c

    def mt_copy(k):
        return remote(zt, ys.at[mine], mt_send, mt_recv, at_y(k, h))

    def sums_over_z():
        landed(zs.at[pl.ds(0, 7)], ms_recv)
        total = zs[0]
        for k in range(1, 8):
            total = total + zs[k]
        zt[...] = total
        for k in range(1, 8):
            mt_copy(k).start()

        @pl.when(first)
        def _():
            ys[mine] = total

        @pl.when(other)
        def _():
            mt_copy(0).start()

    for k in range(1, 5):
        for i in range(NCH):
            y_event(k, i)

            if k < 4:
                @pl.when(first)
                def _():
                    z_event(k, i)
            else:
                @pl.when(other)
                def _():
                    z_start(raw.at[0], i, True).start()
                    z_start(raw.at[0], i, False).start()
            if k == 1 and i < 3:
                spread(i + 1)
            if k == 1 and i == 2:
                for j in range(1, 8):
                    ms_copy(j).start()
        if k == SUMS_AT:
            sums_over_z()

    @pl.when(first)
    def _():
        each(lambda i: landed(raw.at[4, part(i)], y_recv.at[4, i]))
        raw[0] = x_ref[...]

    def wait_mean():
        @pl.when(first)
        def _():
            landed(ys.at[pl.ds(0, 7)], mt_recv)

        @pl.when(other)
        def _():
            landed(ys, mt_recv)

        total = ys[0]
        for k in range(1, 8):
            total = total + ys[k]
        mean[...] = total * (1.0 / NSAMPLES)

    def convert(slot):
        m = mean[...]
        row = jnp.concatenate([m[k : k + 1, :] for k in range(COLS)], axis=1)
        value = raw[slot] - row
        top = value.astype(jnp.bfloat16)
        hl[slot, :ROWS] = top
        hl[slot, ROWS:] = (value - top.astype(jnp.float32)).astype(jnp.bfloat16)

    e_mine = y

    def pair(r, j):
        e_low = rem(e_mine + 8 - r, 8)
        low = 16 * rem(e_low, 4) + 2 * z + div(e_low, 4)
        z_high = rem(z + 8 + j, 8)
        high = 16 * a + 2 * z_high + h
        gap = rem(high + NB - low, NB)
        keep = gap <= HALF
        a_row = jnp.where(keep, rem(e_low, 4), a)
        z_row = jnp.where(keep, z, z_high)
        c_row = jnp.where(keep, div(e_low, 4), h)
        d = jnp.where(keep, gap, NB - gap)
        return keep, gap, (a_row, z_row, c_row), d

    def slot_of(j):
        return jnp.where(j >= 0, jnp.where(j == 0, 0, 4 + j), 8 - j)

    def tile_of(k, t):
        if k == 0:
            return jnp.where(t == 5, 2, t), jnp.int32(0) * t, t == 5
        if k == 4:
            return t, 4 + jnp.int32(0) * t, t < 0
        return jnp.where(t < 5, t, t - 4), jnp.where(t < 5, k, -k), t < 0

    contract = (((1,), (1,)), ((), ()))

    def dot(p, q):
        return lax.dot_general(p, q, contract, preferred_element_type=jnp.float32)

    def compute(k, t):
        r, j, swap = tile_of(k, t)
        keep, _, _, _ = pair(r, j)
        keep = jnp.logical_xor(keep, swap)
        row = jnp.where(keep, r, slot_of(j))
        col = jnp.where(keep, slot_of(j), r)
        both = dot(hl[row], hl[col, :ROWS])
        acc = both[:ROWS] + both[ROWS:] + dot(hl[row, :ROWS], hl[col, ROWS:])
        index = GROUPS[k][0] + t
        for xx in range(4):
            for yy in range(2):
                start = 32 * xx + 16 * yy
                pk[xx, index, yy] = acc[start : start + 16, :]

    def d_copy(k):
        t0, n = GROUPS[k]
        tiles = pl.ds(t0, n)
        return remote(pk.at[:, tiles], pr.at[:, tiles], d_send.at[k], d_recv.at[k], partner)

    def x_copy(k, s):
        t0, n = GROUPS[k]
        return remote(
            pk.at[rem(x + s, 4), pl.ds(t0, n)], xr.at[s - 1, pl.ds(t0, n)],
            x_send.at[k], x_recv.at[k], at_x(s),
        )

    def over_cores(k):
        t0, n = GROUPS[k]
        tiles = pl.ds(t0, n)
        landed(pr.at[:, tiles], d_recv.at[k])
        pk[:, tiles] = pk[:, tiles] + pr[:, tiles]

    def target(k, t):
        r, j, swap = tile_of(k, t)
        keep, gap, (a_row, z_row, c_row), d = pair(r, j)
        valid = jnp.logical_not(jnp.logical_and(swap, gap != HALF))
        low = jnp.logical_and(r == 0, j == 4)
        valid = jnp.logical_and(valid, jnp.logical_or(jnp.logical_not(low), z < 4))
        low = jnp.logical_and(r == 4, j == 0)
        valid = jnp.logical_and(valid, jnp.logical_or(jnp.logical_not(low), h == 0))
        low = jnp.logical_and(r == 4, j == 4)
        valid = jnp.logical_and(valid, jnp.logical_or(jnp.logical_not(low), h == 1))
        a_row = jnp.where(swap, a, a_row)
        z_row = jnp.where(swap, z, z_row)
        c_row = jnp.where(swap, h, c_row)
        mine = (a_row == a) & (z_row == z) & (c_row == c)
        return valid, mine, (a_row, z_row, c_row), d

    def f_copy(k, t, row, d, hh):
        index = GROUPS[k][0] + t
        return remote(
            fb.at[index, hh], out_ref.at[0, d], f_send.at[index], f_recv.at[d], (*row, x, hh)
        )

    def g_copy(t, row, d, xx, hh):
        place = 2 * div(d, 16) + rem(row[2] + d, 2)
        return remote(
            pk.at[xx, GROUPS[4][0] + t, hh], home.at[x, place],
            g_send.at[t], g_recv.at[x, place], (*row, xx, hh),
        )

    def over_planes(k):
        t0, n = GROUPS[k]
        tiles = pl.ds(t0, n)
        landed(xr.at[:, tiles], x_recv.at[k])
        fb[tiles] = (pk[x, tiles] + xr[0, tiles] + xr[1, tiles] + xr[2, tiles]) * (1.0 / NPARAMS)

        def send(t, carry):
            valid, mine, row, d = target(k, t)
            for hh in range(2):
                local = mine & (h == hh)

                @pl.when(jnp.logical_and(valid, local))
                def _():
                    out_ref[0, d] = fb[t0 + t, hh]

                @pl.when(jnp.logical_and(valid, jnp.logical_not(local)))
                def _():
                    f_copy(k, t, row, d, hh).start()

            return carry

        lax.fori_loop(0, n, send, 0)

    def go_home():
        def send(t, carry):
            valid, mine, row, d = target(4, t)
            for xx in range(4):
                for hh in range(2):
                    local = mine & (h == hh) & (x == xx)

                    @pl.when(jnp.logical_and(valid, local))
                    def _():
                        home[xx, 2 * div(d, 16) + rem(row[2] + d, 2)] = pk[xx, GROUPS[4][0] + t, hh]

                    @pl.when(jnp.logical_and(valid, jnp.logical_not(local)))
                    def _():
                        g_copy(t, row, d, xx, hh).start()

            return carry

        lax.fori_loop(0, GROUPS[4][1], send, 0)

    def some(k, start, stop):
        lax.fori_loop(start, stop, lambda t, _: (compute(k, t), 0)[1], 0)

    def convert_round(k):
        if k == 0:
            wait_mean()
            lax.fori_loop(0, 5, lambda s, _: (convert(s), 0)[1], 0)
        elif k < 4:
            convert(UP[k])
            convert(DOWN[k])
        else:
            convert(UP[4])

    @pl.when(other)
    def _():
        for k in range(5):
            n = GROUPS[k][1]
            if k < 4:
                z_event(k + 1, 0)
            if k == 0:
                z_event(1, 1)
            convert_round(k)
            if k == 0:
                z_event(1, 2)
            elif k < 4:
                z_event(k + 1, 1)
            some(k, 0, n // 2)
            if k == 0:
                z_event(1, 3)
            elif k < 4:
                z_event(k + 1, 2)
            some(k, n // 2, n)
            d_copy(k).start()
            if 0 < k < 4:
                z_event(k + 1, 3)

    def plane_sums(k):
        over_cores(k)
        if k < 4:
            for s in range(1, 4):
                x_copy(k, s).start()
        else:
            go_home()

    @pl.when(first)
    def _():
        for k in range(5):
            if k == 4:
                for i in range(NCH):
                    z_event(4, i)
            convert_round(k)
            some(k, 0, GROUPS[k][1])
            if k == 3:
                plane_sums(0)
        for k in range(1, 5):
            plane_sums(k)
            if k > 1:
                over_planes(k - 2)
        over_planes(3)

    @pl.when(first)
    def _():
        remote(x_ref, raw.at[1], own_send.at[0], y_recv.at[1, 0], at_y(1, c)).wait_send()

    @pl.when(other)
    def _():
        for k in range(2):
            remote(x_ref, raw.at[3], own_send.at[k], y_recv.at[3, 0], partner).wait_send()

    for k in range(2):
        remote(x_ref, raw.at[5], z_own.at[k], z_recv.at[0, 0], at_z(1)).wait_send()
    for r in range(1, 4):
        remote(raw.at[r], raw.at[r], y_send.at[r], y_recv.at[r, 0], at_z(1)).wait_send()
    for k in range(1, 4):
        for slot in (UP[k], DOWN[k]):
            piece = raw.at[slot] if k < 3 else raw.at[slot, pl.ds(0, ROWS // 2)]
            remote(piece, piece, z_send.at[slot - 5], z_recv.at[slot - 5, 0], at_z(1)).wait_send()
    remote(zs.at[pl.ds(0, 7)], zs.at[pl.ds(0, 7)], ms_send, ms_recv, at_z(1)).wait_send()

    @pl.when(first)
    def _():
        remote(ys.at[pl.ds(0, 7)], ys.at[pl.ds(0, 7)], mt_send, mt_recv, at_z(1)).wait_send()
        for k in range(4):
            t0, n = GROUPS[k]
            tiles = xr.at[:, pl.ds(t0, n)]
            remote(tiles, tiles, x_send.at[k], x_recv.at[k], at_z(1)).wait_send()

            def gone(t, carry):
                valid, mine, _, _ = target(k, t)

                @pl.when(valid & mine)
                def _():
                    piece = fb.at[0, 0]
                    remote(piece, piece, f_send.at[t0 + t], f_recv.at[0], at_z(1)).wait_send()

                @pl.when(valid & jnp.logical_not(mine))
                def _():
                    pieces = fb.at[0]
                    remote(pieces, pieces, f_send.at[t0 + t], f_recv.at[0], at_z(1)).wait_send()

                return carry

            lax.fori_loop(0, n, gone, 0)

        def left(t, carry):
            valid, mine, _, _ = target(4, t)

            @pl.when(valid & mine)
            def _():
                pieces = pk.at[0, pl.ds(0, 7), 0]
                remote(pieces, pieces, g_send.at[t], g_recv.at[0, 0], at_z(1)).wait_send()

            @pl.when(valid & jnp.logical_not(mine))
            def _():
                pieces = pk.at[0, pl.ds(0, 8), 0]
                remote(pieces, pieces, g_send.at[t], g_recv.at[0, 0], at_z(1)).wait_send()

            return carry

        lax.fori_loop(0, GROUPS[4][1], left, 0)

    @pl.when(other)
    def _():
        remote(ys, ys, mt_send, mt_recv, at_z(1)).wait_send()
        for k in range(5):
            d_copy(k).wait_send()

    def arrived(d, carry):
        step = div(d, 2)
        local = (rem(d, 2) == 0) & (step <= 4) & (z + step <= 7)
        for r in range(1, 5):
            _, gap, _, _ = pair(r, 0)
            here = (gap >= HALF) & (d == NB - gap)
            local = local | ((here & (h == 0)) if r == 4 else here)
        local = local & first
        last = rem(div(rem(16 * a + 2 * z + c + d, NB), 2) + 8 - z, 8) == 4

        @pl.when(jnp.logical_not(last | local))
        def _():
            landed(out_ref.at[0, d], f_recv.at[d])

        return carry

    lax.fori_loop(0, HALF + 1, arrived, 0)

    for place in range(4):
        d = 16 * (place // 2) + 8 + (place % 2) - c
        for xx in range(4):
            @pl.when(jnp.logical_not(first & (d == 8) & (z < 4) & (x == xx)))
            def _():
                landed(home.at[xx, place], g_recv.at[xx, place])
        total = home[0, place] + home[1, place] + home[2, place] + home[3, place]
        out_ref[0, d] = total * (1.0 / NPARAMS)


def on_device(logder):
    f32, bf16 = jnp.float32, jnp.bfloat16
    dma = pltpu.SemaphoreType.DMA
    return pl.pallas_call(
        kernel,
        out_shape=jax.ShapeDtypeStruct((1, HALF + 1, 16, ROWS), f32),
        in_specs=[pl.BlockSpec(memory_space=pltpu.VMEM)],
        out_specs=pl.BlockSpec(memory_space=pltpu.VMEM),
        scratch_shapes=[
            pltpu.VMEM((NSLOT, ROWS, WIDTH), f32),
            pltpu.VMEM((NSLOT, 2 * ROWS, WIDTH), bf16),
            pltpu.VMEM((8, 8, LANES), f32),
            pltpu.VMEM((8, LANES), f32),
            pltpu.VMEM((8, 8, LANES), f32),
            pltpu.VMEM((8, LANES), f32),
            pltpu.VMEM((4, NTILE, 2, 16, ROWS), f32),
            pltpu.VMEM((4, NTILE, 2, 16, ROWS), f32),
            pltpu.VMEM((3, NTILE, 2, 16, ROWS), f32),
            pltpu.VMEM((NTILE, 2, 16, ROWS), f32),
            pltpu.VMEM((4, 4, 16, ROWS), f32),
            dma((2,)),
            dma((5,)),
            dma((5, NCH)),
            dma((7,)),
            dma((2,)),
            dma((7, NCH)),
            dma(()),
            dma(()),
            dma(()),
            dma(()),
            pltpu.SemaphoreType.REGULAR((4,)),
            dma((5,)),
            dma((5,)),
            dma((4,)),
            dma((4,)),
            dma((NTILE,)),
            dma((HALF + 1,)),
            dma((5,)),
            dma((4, 4)),
        ],
        compiler_params=pltpu.CompilerParams(collective_id=0, has_side_effects=True),
    )(logder)


def solution(mesh):
    torus = Mesh(mesh.devices.reshape(4, 8, 2, 4, 2), ("a", "z", "c", "x", "h"))
    return jax.shard_map(
        on_device,
        mesh=torus,
        in_specs=(P(("a", "z", "c"), ("x", "h")),),
        out_specs=P(("a", "z", "c"), None, ("x", "h"), None),
        check_vma=False,
    )
```

```python
import jax
import jax.numpy as jnp
from jax import lax
from jax.experimental import pallas as pl
from jax.experimental.pallas import tpu as pltpu
from jax.sharding import Mesh
from jax.sharding import PartitionSpec as P

MESH = pl.DeviceIdType.MESH

ROWS, WIDTH = 128, 768
LANES = 128
COLS = WIDTH // LANES
NCH = 4
CH = ROWS // NCH
NB = 64
HALF = 32
NSAMPLES = 8192
SUMS_AT = 2
NPARAMS = 6144

NSLOT = 12
UP = {1: 5, 2: 6, 3: 7, 4: 8}
DOWN = {1: 9, 2: 10, 3: 11}

GROUPS = [(0, 6), (6, 8), (14, 8), (22, 8), (30, 5)]
NTILE = 35


def rem(value, count):
    return lax.rem(value, jnp.int32(count))


def div(value, count):
    return lax.div(value, jnp.int32(count))


def kernel(
    x_hbm, out_ref, x_ref, raw, hl, zs, zt, ys, mean, pk, pr, xr, fb, home,
    own_send, y_send, y_recv, z_send, z_own, z_recv, ms_send, ms_recv, mt_send, mt_recv,
    known, x_in, d_send, d_recv, x_send, x_recv, f_send, f_recv, g_send, g_recv,
):
    a = lax.axis_index("a")
    z = lax.axis_index("z")
    c = lax.axis_index("c")
    x = lax.axis_index("x")
    h = lax.axis_index("h")
    y = h * 4 + a
    first = c == h
    other = c != h

    def at_y(steps, core):
        yy = rem(y + 8 + steps, 8)
        return (rem(yy, 4), z, core, x, div(yy, 4))

    def at_z(steps):
        return (a, rem(z + 8 + steps, 8), c, x, h)

    def at_x(steps):
        return (a, z, c, rem(x + steps, 4), h)

    partner = (a, z, 1 - c, x, h)

    def remote(src, dst, send, recv, device):
        return pltpu.make_async_remote_copy(
            src_ref=src, dst_ref=dst, send_sem=send, recv_sem=recv,
            device_id=device, device_id_type=MESH,
        )

    def landed(ref, sem):
        pltpu.make_async_copy(ref, ref, sem).wait()

    fetch = pltpu.make_async_copy(x_hbm, x_ref, x_in)
    fetch.start()

    barrier = pltpu.get_barrier_semaphore()

    def hello(device):
        pl.semaphore_signal(barrier, inc=1, device_id=device, device_id_type=MESH)

    hello(partner)
    for k in (1, 7):
        hello(at_z(k))
        hello(at_y(k, 0))
        hello(at_y(k, 1))
    for k in range(1, 4):
        hello(at_x(k))
    pl.semaphore_wait(barrier, 10)
    fetch.wait()

    def spread(turn):
        if turn > 0:
            for way in range(4):
                pl.semaphore_wait(known.at[way], 1)
        if turn < 3:
            for way, device in enumerate((at_z(1), at_z(-1), at_y(1, c), at_y(-1, c))):
                pl.semaphore_signal(known.at[way], inc=1, device_id=device, device_id_type=MESH)

    def part(i):
        return pl.ds(pl.multiple_of(i * CH, CH), CH)

    def from_below(r):
        return div(rem(y + 8 - r, 8), 4) == c

    def y_own_up(i):
        return remote(x_ref.at[part(i)], raw.at[1, part(i)], own_send.at[0], y_recv.at[1, i], at_y(1, c))

    def y_own_down(i):
        return remote(
            x_ref.at[part(i)], raw.at[3, part(i)], own_send.at[0], y_recv.at[3, i], at_y(-1, 1 - c)
        )

    def y_own_partner(i):
        return remote(x_ref.at[part(i)], raw.at[4, part(i)], own_send.at[1], y_recv.at[4, i], partner)

    def y_relay(r, up, i):
        to = r + 1 if up else r - 1
        return remote(
            raw.at[r, part(i)], raw.at[to, part(i)], y_send.at[r], y_recv.at[to, i],
            at_y(1 if up else -1, c),
        )

    def z_start(src, i, low):
        to = UP[1] if low else DOWN[1]
        return remote(
            src.at[part(i)], raw.at[to, part(i)], z_own.at[0 if low else 1], z_recv.at[to - 5, i],
            at_z(-1 if low else 1),
        )

    def z_relay(slot, to, i, low):
        return remote(
            raw.at[slot, part(i)], raw.at[to, part(i)], z_send.at[slot - 5], z_recv.at[to - 5, i],
            at_z(-1 if low else 1),
        )

    def y_event(dist, i):
        @pl.when(from_below(dist))
        def _():
            landed(raw.at[dist, part(i)], y_recv.at[dist, i])
            if dist < 4:
                y_relay(dist, True, i).start()

        slot = 4 - dist

        @pl.when(jnp.logical_not(from_below(slot)))
        def _():
            landed(raw.at[slot, part(i)], y_recv.at[slot, i])
            if dist < 4:
                y_relay(slot, False, i).start()

    def z_event(k, i):
        if k < 4:
            landed(raw.at[UP[k], part(i)], z_recv.at[UP[k] - 5, i])
            if k < 3:
                z_relay(UP[k], UP[k + 1], i, True).start()
            else:
                if i < NCH // 2:
                    z_relay(UP[3], UP[4], i, True).start()
            landed(raw.at[DOWN[k], part(i)], z_recv.at[DOWN[k] - 5, i])
            if k < 3:
                z_relay(DOWN[k], DOWN[k + 1], i, False).start()
            elif i >= NCH // 2:
                z_relay(DOWN[3], UP[4], i, False).start()
        else:
            landed(raw.at[UP[4], part(i)], z_recv.at[UP[4] - 5, i])

    def each(body):
        lax.fori_loop(0, NCH, lambda i, _: (body(i), 0)[1], 0)

    @pl.when(first)
    def _():
        def go(i):
            y_own_up(i).start()
            z_start(x_ref, i, True).start()
            z_start(x_ref, i, False).start()
        each(go)

    @pl.when(other)
    def _():
        def go(i):
            y_own_down(i).start()
            y_own_partner(i).start()
        each(go)

    spread(0)

    sums = jnp.sum(x_ref[...], axis=0, keepdims=True)
    zs[z] = jnp.zeros((8, LANES), jnp.float32)
    for k in range(COLS):
        zs[z, k : k + 1, :] = sums[:, k * LANES : (k + 1) * LANES]

    def ms_copy(k):
        return remote(zs.at[z], zs.at[z], ms_send, ms_recv, at_z(k))

    mine = 2 * a + c

    def mt_copy(k):
        return remote(zt, ys.at[mine], mt_send, mt_recv, at_y(k, h))

    def sums_over_z():
        landed(zs.at[pl.ds(0, 7)], ms_recv)
        total = zs[0]
        for k in range(1, 8):
            total = total + zs[k]
        zt[...] = total
        for k in range(1, 8):
            mt_copy(k).start()

        @pl.when(first)
        def _():
            ys[mine] = total

        @pl.when(other)
        def _():
            mt_copy(0).start()

    for k in range(1, 5):
        for i in range(NCH):
            y_event(k, i)

            if k < 4:
                @pl.when(first)
                def _():
                    z_event(k, i)
            else:
                @pl.when(other)
                def _():
                    z_start(raw.at[0], i, True).start()
                    z_start(raw.at[0], i, False).start()
            if k == 1 and i < 3:
                spread(i + 1)
            if k == 1 and i == 2:
                for j in range(1, 8):
                    ms_copy(j).start()
        if k == SUMS_AT:
            sums_over_z()

    @pl.when(first)
    def _():
        each(lambda i: landed(raw.at[4, part(i)], y_recv.at[4, i]))
        raw[0] = x_ref[...]

    def wait_mean():
        @pl.when(first)
        def _():
            landed(ys.at[pl.ds(0, 7)], mt_recv)

        @pl.when(other)
        def _():
            landed(ys, mt_recv)

        total = ys[0]
        for k in range(1, 8):
            total = total + ys[k]
        mean[...] = total * (1.0 / NSAMPLES)

    def convert(slot):
        m = mean[...]
        row = jnp.concatenate([m[k : k + 1, :] for k in range(COLS)], axis=1)
        value = raw[slot] - row
        top = value.astype(jnp.bfloat16)
        hl[slot, :ROWS] = top
        hl[slot, ROWS:] = (value - top.astype(jnp.float32)).astype(jnp.bfloat16)

    e_mine = y

    def pair(r, j):
        e_low = rem(e_mine + 8 - r, 8)
        low = 16 * rem(e_low, 4) + 2 * z + div(e_low, 4)
        z_high = rem(z + 8 + j, 8)
        high = 16 * a + 2 * z_high + h
        gap = rem(high + NB - low, NB)
        keep = gap <= HALF
        a_row = jnp.where(keep, rem(e_low, 4), a)
        z_row = jnp.where(keep, z, z_high)
        c_row = jnp.where(keep, div(e_low, 4), h)
        d = jnp.where(keep, gap, NB - gap)
        return keep, gap, (a_row, z_row, c_row), d

    def slot_of(j):
        return jnp.where(j >= 0, jnp.where(j == 0, 0, 4 + j), 8 - j)

    def tile_of(k, t):
        if k == 0:
            return jnp.where(t == 5, 2, t), jnp.int32(0) * t, t == 5
        if k == 4:
            return t, 4 + jnp.int32(0) * t, t < 0
        return jnp.where(t < 5, t, t - 4), jnp.where(t < 5, k, -k), t < 0

    contract = (((1,), (1,)), ((), ()))

    def dot(p, q):
        return lax.dot_general(p, q, contract, preferred_element_type=jnp.float32)

    def put(index, acc):
        for xx in range(4):
            for yy in range(2):
                start = 32 * xx + 16 * yy
                pk[xx, index, yy] = acc[start : start + 16, :]

    def compute(k, p):
        low, high = (0, 5) if p == 0 else (1, 4)
        j = k if p == 0 else -k
        slot = 0 if k == 0 else (UP[k] if p == 0 else DOWN[k])
        n = high - low
        tops = hl[low:high, :ROWS].reshape(n * ROWS, WIDTH)
        rests = hl[low:high, ROWS:].reshape(n * ROWS, WIDTH)
        both = dot(tops, hl[slot])
        acc = both[:, :ROWS] + both[:, ROWS:] + dot(rests, hl[slot, :ROWS])
        for r in range(low, high):
            tile = acc[(r - low) * ROWS : (r - low + 1) * ROWS]
            index = GROUPS[k][0] + (r if p == 0 else r + 4)
            keep, _, _, _ = pair(r, j)

            @pl.when(keep)
            def _():
                put(index, tile)

            @pl.when(jnp.logical_not(keep))
            def _():
                put(index, tile.T)

            if k == 0 and r == 2:
                put(GROUPS[0][0] + 5, tile.T)

    def some_tiles(k, p):
        t0, n = GROUPS[k]
        if k in (0, 4):
            return pl.ds(t0, n)
        return pl.ds(t0, 5) if p == 0 else pl.ds(t0 + 5, 3)

    def d_copy(k, p):
        tiles = some_tiles(k, p)
        return remote(pk.at[:, tiles], pr.at[:, tiles], d_send.at[k, p], d_recv.at[k, p], partner)

    def x_copy(k, p, s):
        tiles = some_tiles(k, p)
        return remote(
            pk.at[rem(x + s, 4), tiles], xr.at[s - 1, tiles], x_send.at[k, p], x_recv.at[k, p], at_x(s)
        )

    def over_cores(k, p):
        tiles = some_tiles(k, p)
        landed(pr.at[:, tiles], d_recv.at[k, p])
        pk[:, tiles] = pk[:, tiles] + pr[:, tiles]

    def target(k, t):
        r, j, swap = tile_of(k, t)
        keep, gap, (a_row, z_row, c_row), d = pair(r, j)
        valid = jnp.logical_not(jnp.logical_and(swap, gap != HALF))
        low = jnp.logical_and(r == 0, j == 4)
        valid = jnp.logical_and(valid, jnp.logical_or(jnp.logical_not(low), z < 4))
        low = jnp.logical_and(r == 4, j == 0)
        valid = jnp.logical_and(valid, jnp.logical_or(jnp.logical_not(low), h == 0))
        low = jnp.logical_and(r == 4, j == 4)
        valid = jnp.logical_and(valid, jnp.logical_or(jnp.logical_not(low), h == 1))
        a_row = jnp.where(swap, a, a_row)
        z_row = jnp.where(swap, z, z_row)
        c_row = jnp.where(swap, h, c_row)
        mine = (a_row == a) & (z_row == z) & (c_row == c)
        return valid, mine, (a_row, z_row, c_row), d

    def f_copy(k, t, row, d, hh):
        index = GROUPS[k][0] + t
        return remote(
            fb.at[index, hh], out_ref.at[0, d], f_send.at[index], f_recv.at[d], (*row, x, hh)
        )

    def g_copy(t, row, d, xx, hh):
        place = 2 * div(d, 16) + rem(row[2] + d, 2)
        return remote(
            pk.at[xx, GROUPS[4][0] + t, hh], home.at[x, place],
            g_send.at[t], g_recv.at[x, place], (*row, xx, hh),
        )

    def over_planes(k, p):
        t0, _ = GROUPS[k]
        tiles = some_tiles(k, p)
        landed(xr.at[:, tiles], x_recv.at[k, p])
        fb[tiles] = (pk[x, tiles] + xr[0, tiles] + xr[1, tiles] + xr[2, tiles]) * (1.0 / NPARAMS)

        def send(t, carry):
            valid, mine, row, d = target(k, t)
            for hh in range(2):
                local = mine & (h == hh)

                @pl.when(jnp.logical_and(valid, local))
                def _():
                    out_ref[0, d] = fb[t0 + t, hh]

                @pl.when(jnp.logical_and(valid, jnp.logical_not(local)))
                def _():
                    f_copy(k, t, row, d, hh).start()

            return carry

        if k == 0:
            lax.fori_loop(0, 6, send, 0)
        else:
            lax.fori_loop(5 * p, 5 + 3 * p, send, 0)

    def go_home():
        def send(t, carry):
            valid, mine, row, d = target(4, t)
            for xx in range(4):
                for hh in range(2):
                    local = mine & (h == hh) & (x == xx)

                    @pl.when(jnp.logical_and(valid, local))
                    def _():
                        home[xx, 2 * div(d, 16) + rem(row[2] + d, 2)] = pk[xx, GROUPS[4][0] + t, hh]

                    @pl.when(jnp.logical_and(valid, jnp.logical_not(local)))
                    def _():
                        g_copy(t, row, d, xx, hh).start()

            return carry

        lax.fori_loop(0, GROUPS[4][1], send, 0)

    def convert_first():
        wait_mean()
        lax.fori_loop(0, 5, lambda s, _: (convert(s), 0)[1], 0)

    @pl.when(other)
    def _():
        for i in range(2):
            z_event(1, i)
        convert_first()
        for i in range(2, 4):
            z_event(1, i)
        compute(0, 0)
        d_copy(0, 0).start()
        for k in range(1, 4):
            z_event(k + 1, 0)
            convert(UP[k])
            z_event(k + 1, 1)
            compute(k, 0)
            d_copy(k, 0).start()
            z_event(k + 1, 2)
            convert(DOWN[k])
            compute(k, 1)
            d_copy(k, 1).start()
            z_event(k + 1, 3)
        convert(UP[4])
        compute(4, 0)
        over_cores(4, 0)
        go_home()

    def plane_sums(k, p):
        over_cores(k, p)
        for s in range(1, 4):
            x_copy(k, p, s).start()

    @pl.when(first)
    def _():
        convert_first()
        compute(0, 0)
        for k in range(1, 4):
            convert(UP[k])
            convert(DOWN[k])
            compute(k, 0)
            compute(k, 1)
        plane_sums(0, 0)
        for i in range(NCH):
            z_event(4, i)
        convert(UP[4])
        compute(4, 0)
        d_copy(4, 0).start()
        plane_sums(1, 0)
        plane_sums(1, 1)
        plane_sums(2, 0)
        over_planes(0, 0)
        plane_sums(2, 1)
        over_planes(1, 0)
        over_planes(1, 1)
        plane_sums(3, 0)
        plane_sums(3, 1)
        over_planes(2, 0)
        over_planes(2, 1)
        over_planes(3, 0)
        over_planes(3, 1)

    @pl.when(first)
    def _():
        remote(x_ref, raw.at[1], own_send.at[0], y_recv.at[1, 0], at_y(1, c)).wait_send()

    @pl.when(other)
    def _():
        for k in range(2):
            remote(x_ref, raw.at[3], own_send.at[k], y_recv.at[3, 0], partner).wait_send()

    for k in range(2):
        remote(x_ref, raw.at[5], z_own.at[k], z_recv.at[0, 0], at_z(1)).wait_send()
    for r in range(1, 4):
        remote(raw.at[r], raw.at[r], y_send.at[r], y_recv.at[r, 0], at_z(1)).wait_send()
    for k in range(1, 4):
        for slot in (UP[k], DOWN[k]):
            piece = raw.at[slot] if k < 3 else raw.at[slot, pl.ds(0, ROWS // 2)]
            remote(piece, piece, z_send.at[slot - 5], z_recv.at[slot - 5, 0], at_z(1)).wait_send()
    remote(zs.at[pl.ds(0, 7)], zs.at[pl.ds(0, 7)], ms_send, ms_recv, at_z(1)).wait_send()

    @pl.when(first)
    def _():
        remote(ys.at[pl.ds(0, 7)], ys.at[pl.ds(0, 7)], mt_send, mt_recv, at_z(1)).wait_send()
        for k in range(4):
            t0, n = GROUPS[k]
            for p in range(2 if k else 1):
                tiles = xr.at[:, some_tiles(k, p)]
                remote(tiles, tiles, x_send.at[k, p], x_recv.at[k, p], at_z(1)).wait_send()

            def gone(t, carry):
                valid, mine, _, _ = target(k, t)

                @pl.when(valid & mine)
                def _():
                    piece = fb.at[0, 0]
                    remote(piece, piece, f_send.at[t0 + t], f_recv.at[0], at_z(1)).wait_send()

                @pl.when(valid & jnp.logical_not(mine))
                def _():
                    pieces = fb.at[0]
                    remote(pieces, pieces, f_send.at[t0 + t], f_recv.at[0], at_z(1)).wait_send()

                return carry

            lax.fori_loop(0, n, gone, 0)
        d_copy(4, 0).wait_send()

    @pl.when(other)
    def _():
        remote(ys, ys, mt_send, mt_recv, at_z(1)).wait_send()
        for k in range(4):
            for p in range(2 if k else 1):
                d_copy(k, p).wait_send()

        def left(t, carry):
            valid, mine, _, _ = target(4, t)

            @pl.when(valid & mine)
            def _():
                pieces = pk.at[0, pl.ds(0, 7), 0]
                remote(pieces, pieces, g_send.at[t], g_recv.at[0, 0], at_z(1)).wait_send()

            @pl.when(valid & jnp.logical_not(mine))
            def _():
                pieces = pk.at[0, pl.ds(0, 8), 0]
                remote(pieces, pieces, g_send.at[t], g_recv.at[0, 0], at_z(1)).wait_send()

            return carry

        lax.fori_loop(0, GROUPS[4][1], left, 0)

    def arrived(d, carry):
        step = div(d, 2)
        local = (rem(d, 2) == 0) & (step <= 4) & (z + step <= 7)
        for r in range(1, 5):
            _, gap, _, _ = pair(r, 0)
            here = (gap >= HALF) & (d == NB - gap)
            local = local | ((here & (h == 0)) if r == 4 else here)
        local = local & first
        last = rem(div(rem(16 * a + 2 * z + c + d, NB), 2) + 8 - z, 8) == 4

        @pl.when(jnp.logical_not(last | local))
        def _():
            landed(out_ref.at[0, d], f_recv.at[d])

        return carry

    lax.fori_loop(0, HALF + 1, arrived, 0)

    for place in range(4):
        d = 16 * (place // 2) + 8 + (place % 2) - c
        for xx in range(4):
            @pl.when(jnp.logical_not(other & (d == 9) & (h == 1) & (z < 4) & (x == xx)))
            def _():
                landed(home.at[xx, place], g_recv.at[xx, place])
        total = home[0, place] + home[1, place] + home[2, place] + home[3, place]
        out_ref[0, d] = total * (1.0 / NPARAMS)


def on_device(logder):
    f32, bf16 = jnp.float32, jnp.bfloat16
    dma = pltpu.SemaphoreType.DMA
    return pl.pallas_call(
        kernel,
        out_shape=jax.ShapeDtypeStruct((1, HALF + 1, 16, ROWS), f32),
        in_specs=[pl.BlockSpec(memory_space=pl.ANY)],
        out_specs=pl.BlockSpec(memory_space=pltpu.VMEM),
        scratch_shapes=[
            pltpu.VMEM((ROWS, WIDTH), f32),
            pltpu.VMEM((NSLOT, ROWS, WIDTH), f32),
            pltpu.VMEM((NSLOT, 2 * ROWS, WIDTH), bf16),
            pltpu.VMEM((8, 8, LANES), f32),
            pltpu.VMEM((8, LANES), f32),
            pltpu.VMEM((8, 8, LANES), f32),
            pltpu.VMEM((8, LANES), f32),
            pltpu.VMEM((4, NTILE, 2, 16, ROWS), f32),
            pltpu.VMEM((4, NTILE, 2, 16, ROWS), f32),
            pltpu.VMEM((3, NTILE, 2, 16, ROWS), f32),
            pltpu.VMEM((NTILE, 2, 16, ROWS), f32),
            pltpu.VMEM((4, 4, 16, ROWS), f32),
            dma((2,)),
            dma((5,)),
            dma((5, NCH)),
            dma((7,)),
            dma((2,)),
            dma((7, NCH)),
            dma(()),
            dma(()),
            dma(()),
            dma(()),
            pltpu.SemaphoreType.REGULAR((4,)),
            dma(()),
            dma((5, 2)),
            dma((5, 2)),
            dma((4, 2)),
            dma((4, 2)),
            dma((NTILE,)),
            dma((HALF + 1,)),
            dma((5,)),
            dma((4, 4)),
        ],
        compiler_params=pltpu.CompilerParams(collective_id=0, has_side_effects=True),
    )(logder)


def solution(mesh):
    torus = Mesh(mesh.devices.reshape(4, 8, 2, 4, 2), ("a", "z", "c", "x", "h"))
    return jax.shard_map(
        on_device,
        mesh=torus,
        in_specs=(P(("a", "z", "c"), ("x", "h")),),
        out_specs=P(("a", "z", "c"), None, ("x", "h"), None),
        check_vma=False,
    )
```

```python
import jax
import jax.numpy as jnp
from jax import lax
from jax.experimental import pallas as pl
from jax.experimental.pallas import tpu as pltpu
from jax.sharding import Mesh
from jax.sharding import PartitionSpec as P

MESH = pl.DeviceIdType.MESH

ROWS, WIDTH = 128, 768
LANES = 128
COLS = WIDTH // LANES
NCH = 4
CH = ROWS // NCH
NB = 64
HALF = 32
NSAMPLES = 8192
SUMS_AT = 2
NPARAMS = 6144

NSLOT = 12
UP = {1: 5, 2: 6, 3: 7, 4: 8}
DOWN = {1: 9, 2: 10, 3: 11}

GROUPS = [(0, 6), (6, 8), (14, 8), (22, 8), (30, 5)]
NTILE = 35


def rem(value, count):
    return lax.rem(value, jnp.int32(count))


def div(value, count):
    return lax.div(value, jnp.int32(count))


def kernel(
    x_hbm, out_ref, x_ref, raw, hl, zs, zt, ys, mean, pk, pr, xr, fb, home,
    own_send, y_send, y_recv, z_send, z_own, z_recv, ms_send, ms_recv, mt_send, mt_recv,
    known, x_in, d_send, d_recv, x_send, x_recv, f_send, f_recv, g_send, g_recv,
):
    a = lax.axis_index("a")
    z = lax.axis_index("z")
    c = lax.axis_index("c")
    x = lax.axis_index("x")
    h = lax.axis_index("h")
    y = h * 4 + a
    first = c == h
    other = c != h

    def at_y(steps, core):
        yy = rem(y + 8 + steps, 8)
        return (rem(yy, 4), z, core, x, div(yy, 4))

    def at_z(steps):
        return (a, rem(z + 8 + steps, 8), c, x, h)

    def at_x(steps):
        return (a, z, c, rem(x + steps, 4), h)

    partner = (a, z, 1 - c, x, h)

    def remote(src, dst, send, recv, device):
        return pltpu.make_async_remote_copy(
            src_ref=src, dst_ref=dst, send_sem=send, recv_sem=recv,
            device_id=device, device_id_type=MESH,
        )

    def landed(ref, sem):
        pltpu.make_async_copy(ref, ref, sem).wait()

    fetch = pltpu.make_async_copy(x_hbm, x_ref, x_in)
    fetch.start()

    barrier = pltpu.get_barrier_semaphore()

    def hello(device):
        pl.semaphore_signal(barrier, inc=1, device_id=device, device_id_type=MESH)

    hello(partner)
    for k in (1, 7):
        hello(at_z(k))
        hello(at_y(k, 0))
        hello(at_y(k, 1))
    for k in range(1, 4):
        hello(at_x(k))
    pl.semaphore_wait(barrier, 10)
    fetch.wait()

    def spread(turn):
        if turn > 0:
            for way in range(4):
                pl.semaphore_wait(known.at[way], 1)
        if turn < 3:
            for way, device in enumerate((at_z(1), at_z(-1), at_y(1, c), at_y(-1, c))):
                pl.semaphore_signal(known.at[way], inc=1, device_id=device, device_id_type=MESH)

    def part(i):
        return pl.ds(pl.multiple_of(i * CH, CH), CH)

    def from_below(r):
        return div(rem(y + 8 - r, 8), 4) == c

    def y_own_up(i):
        return remote(x_ref.at[part(i)], raw.at[1, part(i)], own_send.at[0], y_recv.at[1, i], at_y(1, c))

    def y_own_down(i):
        return remote(
            x_ref.at[part(i)], raw.at[3, part(i)], own_send.at[0], y_recv.at[3, i], at_y(-1, 1 - c)
        )

    def y_own_partner(i):
        return remote(x_ref.at[part(i)], raw.at[4, part(i)], own_send.at[1], y_recv.at[4, i], partner)

    def y_relay(r, up, i):
        to = r + 1 if up else r - 1
        return remote(
            raw.at[r, part(i)], raw.at[to, part(i)], y_send.at[r], y_recv.at[to, i],
            at_y(1 if up else -1, c),
        )

    def z_start(src, i, low):
        to = UP[1] if low else DOWN[1]
        return remote(
            src.at[part(i)], raw.at[to, part(i)], z_own.at[0 if low else 1], z_recv.at[to - 5, i],
            at_z(-1 if low else 1),
        )

    def z_relay(slot, to, i, low):
        return remote(
            raw.at[slot, part(i)], raw.at[to, part(i)], z_send.at[slot - 5], z_recv.at[to - 5, i],
            at_z(-1 if low else 1),
        )

    def y_event(dist, i):
        @pl.when(from_below(dist))
        def _():
            landed(raw.at[dist, part(i)], y_recv.at[dist, i])
            if dist < 4:
                y_relay(dist, True, i).start()

        slot = 4 - dist

        @pl.when(jnp.logical_not(from_below(slot)))
        def _():
            landed(raw.at[slot, part(i)], y_recv.at[slot, i])
            if dist < 4:
                y_relay(slot, False, i).start()

    def z_event(k, i):
        if k < 4:
            landed(raw.at[UP[k], part(i)], z_recv.at[UP[k] - 5, i])
            if k < 3:
                z_relay(UP[k], UP[k + 1], i, True).start()
            else:
                if i < NCH // 2:
                    z_relay(UP[3], UP[4], i, True).start()
            landed(raw.at[DOWN[k], part(i)], z_recv.at[DOWN[k] - 5, i])
            if k < 3:
                z_relay(DOWN[k], DOWN[k + 1], i, False).start()
            elif i >= NCH // 2:
                z_relay(DOWN[3], UP[4], i, False).start()
        else:
            landed(raw.at[UP[4], part(i)], z_recv.at[UP[4] - 5, i])

    def each(body):
        lax.fori_loop(0, NCH, lambda i, _: (body(i), 0)[1], 0)

    @pl.when(first)
    def _():
        def go(i):
            y_own_up(i).start()
            z_start(x_ref, i, True).start()
            z_start(x_ref, i, False).start()
        each(go)

    @pl.when(other)
    def _():
        def go(i):
            y_own_down(i).start()
            y_own_partner(i).start()
        each(go)

    spread(0)

    sums = jnp.sum(x_ref[...], axis=0, keepdims=True)
    zs[z] = jnp.zeros((8, LANES), jnp.float32)
    for k in range(COLS):
        zs[z, k : k + 1, :] = sums[:, k * LANES : (k + 1) * LANES]

    def ms_copy(k):
        return remote(zs.at[z], zs.at[z], ms_send, ms_recv, at_z(k))

    mine = 2 * a + c

    def mt_copy(k):
        return remote(zt, ys.at[mine], mt_send, mt_recv, at_y(k, h))

    def sums_over_z():
        landed(zs.at[pl.ds(0, 7)], ms_recv)
        total = zs[0]
        for k in range(1, 8):
            total = total + zs[k]
        zt[...] = total
        for k in range(1, 8):
            mt_copy(k).start()

        @pl.when(first)
        def _():
            ys[mine] = total

        @pl.when(other)
        def _():
            mt_copy(0).start()

    for k in range(1, 5):
        for i in range(NCH):
            y_event(k, i)

            if k < 4:
                @pl.when(first)
                def _():
                    z_event(k, i)
            else:
                @pl.when(other)
                def _():
                    z_start(raw.at[0], i, True).start()
                    z_start(raw.at[0], i, False).start()
            if k == 1 and i < 3:
                spread(i + 1)
            if k == 1 and i == 2:
                for j in range(1, 8):
                    ms_copy(j).start()
        if k == SUMS_AT:
            sums_over_z()

    @pl.when(first)
    def _():
        each(lambda i: landed(raw.at[4, part(i)], y_recv.at[4, i]))
        raw[0] = x_ref[...]

    def wait_mean():
        @pl.when(first)
        def _():
            landed(ys.at[pl.ds(0, 7)], mt_recv)

        @pl.when(other)
        def _():
            landed(ys, mt_recv)

        total = ys[0]
        for k in range(1, 8):
            total = total + ys[k]
        mean[...] = total * (1.0 / NSAMPLES)

    def convert(slot):
        m = mean[...]
        row = jnp.concatenate([m[k : k + 1, :] for k in range(COLS)], axis=1)
        value = raw[slot] - row
        top = value.astype(jnp.bfloat16)
        hl[slot, :ROWS] = top
        hl[slot, ROWS:] = (value - top.astype(jnp.float32)).astype(jnp.bfloat16)

    e_mine = y

    def pair(r, j):
        e_low = rem(e_mine + 8 - r, 8)
        low = 16 * rem(e_low, 4) + 2 * z + div(e_low, 4)
        z_high = rem(z + 8 + j, 8)
        high = 16 * a + 2 * z_high + h
        gap = rem(high + NB - low, NB)
        keep = gap <= HALF
        a_row = jnp.where(keep, rem(e_low, 4), a)
        z_row = jnp.where(keep, z, z_high)
        c_row = jnp.where(keep, div(e_low, 4), h)
        d = jnp.where(keep, gap, NB - gap)
        return keep, gap, (a_row, z_row, c_row), d

    def slot_of(j):
        return jnp.where(j >= 0, jnp.where(j == 0, 0, 4 + j), 8 - j)

    def tile_of(k, t):
        if k == 0:
            return jnp.where(t == 5, 2, t), jnp.int32(0) * t, t == 5
        if k == 4:
            return t, 4 + jnp.int32(0) * t, t < 0
        return jnp.where(t < 5, t, t - 4), jnp.where(t < 5, k, -k), t < 0

    contract = (((1,), (1,)), ((), ()))

    def dot(p, q):
        return lax.dot_general(p, q, contract, preferred_element_type=jnp.float32)

    def put(index, acc):
        for xx in range(4):
            for yy in range(2):
                start = 32 * xx + 16 * yy
                pk[xx, index, yy] = acc[start : start + 16, :]

    def compute(k, p):
        low, high = (0, 5) if p == 0 else (1, 4)
        j = k if p == 0 else -k
        slot = 0 if k == 0 else (UP[k] if p == 0 else DOWN[k])
        n = high - low
        tops = hl[low:high, :ROWS].reshape(n * ROWS, WIDTH)
        rests = hl[low:high, ROWS:].reshape(n * ROWS, WIDTH)
        both = dot(tops, hl[slot])
        acc = both[:, :ROWS] + both[:, ROWS:] + dot(rests, hl[slot, :ROWS])
        for r in range(low, high):
            tile = acc[(r - low) * ROWS : (r - low + 1) * ROWS]
            index = GROUPS[k][0] + (r if p == 0 else r + 4)
            keep, _, _, _ = pair(r, j)

            @pl.when(keep)
            def _():
                put(index, tile)

            @pl.when(jnp.logical_not(keep))
            def _():
                put(index, tile.T)

            if k == 0 and r == 2:
                put(GROUPS[0][0] + 5, tile.T)

    def some_tiles(k, p):
        t0, n = GROUPS[k]
        if k in (0, 4):
            return pl.ds(t0, n)
        return pl.ds(t0, 5) if p == 0 else pl.ds(t0 + 5, 3)

    def d_copy(k, p):
        tiles = some_tiles(k, p)
        return remote(pk.at[:, tiles], pr.at[:, tiles], d_send.at[k, p], d_recv.at[k, p], partner)

    def x_copy(k, p, s):
        tiles = some_tiles(k, p)
        return remote(
            pk.at[rem(x + s, 4), tiles], xr.at[s - 1, tiles], x_send.at[k, p], x_recv.at[k, p], at_x(s)
        )

    def over_cores(k, p):
        tiles = some_tiles(k, p)
        landed(pr.at[:, tiles], d_recv.at[k, p])
        pk[:, tiles] = pk[:, tiles] + pr[:, tiles]

    def target(k, t):
        r, j, swap = tile_of(k, t)
        keep, gap, (a_row, z_row, c_row), d = pair(r, j)
        valid = jnp.logical_not(jnp.logical_and(swap, gap != HALF))
        low = jnp.logical_and(r == 0, j == 4)
        valid = jnp.logical_and(valid, jnp.logical_or(jnp.logical_not(low), z < 4))
        low = jnp.logical_and(r == 4, j == 0)
        valid = jnp.logical_and(valid, jnp.logical_or(jnp.logical_not(low), h == 0))
        low = jnp.logical_and(r == 4, j == 4)
        valid = jnp.logical_and(valid, jnp.logical_or(jnp.logical_not(low), h == 1))
        a_row = jnp.where(swap, a, a_row)
        z_row = jnp.where(swap, z, z_row)
        c_row = jnp.where(swap, h, c_row)
        mine = (a_row == a) & (z_row == z) & (c_row == c)
        return valid, mine, (a_row, z_row, c_row), d

    def f_copy(k, t, row, d, hh):
        index = GROUPS[k][0] + t
        return remote(
            fb.at[index, hh], out_ref.at[0, d], f_send.at[index], f_recv.at[d], (*row, x, hh)
        )

    def g_copy(t, row, d, xx, hh):
        place = 2 * div(d, 16) + rem(row[2] + d, 2)
        return remote(
            pk.at[xx, GROUPS[4][0] + t, hh], home.at[x, place],
            g_send.at[t], g_recv.at[x, place], (*row, xx, hh),
        )

    def over_planes(k, p):
        t0, _ = GROUPS[k]
        tiles = some_tiles(k, p)
        landed(xr.at[:, tiles], x_recv.at[k, p])
        fb[tiles] = (pk[x, tiles] + xr[0, tiles] + xr[1, tiles] + xr[2, tiles]) * (1.0 / NPARAMS)

        def send(t, carry):
            valid, mine, row, d = target(k, t)
            for hh in range(2):
                local = mine & (h == hh)

                @pl.when(jnp.logical_and(valid, local))
                def _():
                    out_ref[0, d] = fb[t0 + t, hh]

                @pl.when(jnp.logical_and(valid, jnp.logical_not(local)))
                def _():
                    f_copy(k, t, row, d, hh).start()

            return carry

        if k == 0:
            lax.fori_loop(0, 6, send, 0)
        else:
            lax.fori_loop(5 * p, 5 + 3 * p, send, 0)

    def go_home():
        def send(t, carry):
            valid, mine, row, d = target(4, t)
            for xx in range(4):
                for hh in range(2):
                    local = mine & (h == hh) & (x == xx)

                    @pl.when(jnp.logical_and(valid, local))
                    def _():
                        home[xx, 2 * div(d, 16) + rem(row[2] + d, 2)] = pk[xx, GROUPS[4][0] + t, hh]

                    @pl.when(jnp.logical_and(valid, jnp.logical_not(local)))
                    def _():
                        g_copy(t, row, d, xx, hh).start()

            return carry

        lax.fori_loop(0, GROUPS[4][1], send, 0)

    def convert_first():
        wait_mean()
        lax.fori_loop(0, 5, lambda s, _: (convert(s), 0)[1], 0)

    @pl.when(other)
    def _():
        for i in range(2):
            z_event(1, i)
        convert_first()
        for i in range(2, 4):
            z_event(1, i)
        compute(0, 0)
        d_copy(0, 0).start()
        for k in range(1, 4):
            z_event(k + 1, 0)
            convert(UP[k])
            z_event(k + 1, 1)
            compute(k, 0)
            d_copy(k, 0).start()
            z_event(k + 1, 2)
            convert(DOWN[k])
            compute(k, 1)
            d_copy(k, 1).start()
            z_event(k + 1, 3)
        convert(UP[4])
        compute(4, 0)
        over_cores(4, 0)
        go_home()

    def plane_sums(k, p):
        over_cores(k, p)
        for s in range(1, 4):
            x_copy(k, p, s).start()

    @pl.when(first)
    def _():
        convert_first()
        compute(0, 0)
        for k in range(1, 4):
            convert(UP[k])
            convert(DOWN[k])
            compute(k, 0)
            compute(k, 1)
        plane_sums(0, 0)
        for i in range(NCH):
            z_event(4, i)
        convert(UP[4])
        compute(4, 0)
        d_copy(4, 0).start()
        plane_sums(1, 0)
        plane_sums(1, 1)
        plane_sums(2, 0)
        over_planes(0, 0)
        plane_sums(2, 1)
        over_planes(1, 0)
        over_planes(1, 1)
        plane_sums(3, 0)
        plane_sums(3, 1)
        over_planes(2, 0)
        over_planes(2, 1)
        over_planes(3, 0)
        over_planes(3, 1)

    @pl.when(first)
    def _():
        remote(x_ref, raw.at[1], own_send.at[0], y_recv.at[1, 0], at_y(1, c)).wait_send()

    @pl.when(other)
    def _():
        for k in range(2):
            remote(x_ref, raw.at[3], own_send.at[k], y_recv.at[3, 0], partner).wait_send()

    for k in range(2):
        remote(x_ref, raw.at[5], z_own.at[k], z_recv.at[0, 0], at_z(1)).wait_send()
    for r in range(1, 4):
        remote(raw.at[r], raw.at[r], y_send.at[r], y_recv.at[r, 0], at_z(1)).wait_send()
    for k in range(1, 4):
        for slot in (UP[k], DOWN[k]):
            piece = raw.at[slot] if k < 3 else raw.at[slot, pl.ds(0, ROWS // 2)]
            remote(piece, piece, z_send.at[slot - 5], z_recv.at[slot - 5, 0], at_z(1)).wait_send()
    remote(zs.at[pl.ds(0, 7)], zs.at[pl.ds(0, 7)], ms_send, ms_recv, at_z(1)).wait_send()

    @pl.when(first)
    def _():
        remote(ys.at[pl.ds(0, 7)], ys.at[pl.ds(0, 7)], mt_send, mt_recv, at_z(1)).wait_send()
        for k in range(4):
            t0, n = GROUPS[k]
            for p in range(2 if k else 1):
                tiles = xr.at[:, some_tiles(k, p)]
                remote(tiles, tiles, x_send.at[k, p], x_recv.at[k, p], at_z(1)).wait_send()

            def gone(t, carry):
                valid, mine, _, _ = target(k, t)

                @pl.when(valid & mine)
                def _():
                    piece = fb.at[0, 0]
                    remote(piece, piece, f_send.at[t0 + t], f_recv.at[0], at_z(1)).wait_send()

                @pl.when(valid & jnp.logical_not(mine))
                def _():
                    pieces = fb.at[0]
                    remote(pieces, pieces, f_send.at[t0 + t], f_recv.at[0], at_z(1)).wait_send()

                return carry

            lax.fori_loop(0, n, gone, 0)
        d_copy(4, 0).wait_send()

    @pl.when(other)
    def _():
        remote(ys, ys, mt_send, mt_recv, at_z(1)).wait_send()
        for k in range(4):
            for p in range(2 if k else 1):
                d_copy(k, p).wait_send()

        def left(t, carry):
            valid, mine, _, _ = target(4, t)

            @pl.when(valid & mine)
            def _():
                pieces = pk.at[0, pl.ds(0, 7), 0]
                remote(pieces, pieces, g_send.at[t], g_recv.at[0, 0], at_z(1)).wait_send()

            @pl.when(valid & jnp.logical_not(mine))
            def _():
                pieces = pk.at[0, pl.ds(0, 8), 0]
                remote(pieces, pieces, g_send.at[t], g_recv.at[0, 0], at_z(1)).wait_send()

            return carry

        lax.fori_loop(0, GROUPS[4][1], left, 0)

    def arrived(d, carry):
        step = div(d, 2)
        local = (rem(d, 2) == 0) & (step <= 4) & (z + step <= 7)
        for r in range(1, 5):
            _, gap, _, _ = pair(r, 0)
            here = (gap >= HALF) & (d == NB - gap)
            local = local | ((here & (h == 0)) if r == 4 else here)
        local = local & first
        last = rem(div(rem(16 * a + 2 * z + c + d, NB), 2) + 8 - z, 8) == 4

        @pl.when(jnp.logical_not(last | local))
        def _():
            landed(out_ref.at[0, d], f_recv.at[d])

        return carry

    lax.fori_loop(0, HALF + 1, arrived, 0)

    for place in range(4):
        d = 16 * (place // 2) + 8 + (place % 2) - c
        for xx in range(4):
            @pl.when(jnp.logical_not(other & (d == 9) & (h == 1) & (z < 4) & (x == xx)))
            def _():
                landed(home.at[xx, place], g_recv.at[xx, place])
        total = home[0, place] + home[1, place] + home[2, place] + home[3, place]
        out_ref[0, d] = total * (1.0 / NPARAMS)


def on_device(logder):
    f32, bf16 = jnp.float32, jnp.bfloat16
    dma = pltpu.SemaphoreType.DMA
    return pl.pallas_call(
        kernel,
        out_shape=pltpu.VMEM((1, HALF + 1, 16, ROWS), f32),
        in_specs=[pl.BlockSpec(memory_space=pl.ANY)],
        out_specs=pl.BlockSpec(memory_space=pltpu.VMEM),
        scratch_shapes=[
            pltpu.VMEM((ROWS, WIDTH), f32),
            pltpu.VMEM((NSLOT, ROWS, WIDTH), f32),
            pltpu.VMEM((NSLOT, 2 * ROWS, WIDTH), bf16),
            pltpu.VMEM((8, 8, LANES), f32),
            pltpu.VMEM((8, LANES), f32),
            pltpu.VMEM((8, 8, LANES), f32),
            pltpu.VMEM((8, LANES), f32),
            pltpu.VMEM((4, NTILE, 2, 16, ROWS), f32),
            pltpu.VMEM((4, NTILE, 2, 16, ROWS), f32),
            pltpu.VMEM((3, NTILE, 2, 16, ROWS), f32),
            pltpu.VMEM((NTILE, 2, 16, ROWS), f32),
            pltpu.VMEM((4, 4, 16, ROWS), f32),
            dma((2,)),
            dma((5,)),
            dma((5, NCH)),
            dma((7,)),
            dma((2,)),
            dma((7, NCH)),
            dma(()),
            dma(()),
            dma(()),
            dma(()),
            pltpu.SemaphoreType.REGULAR((4,)),
            dma(()),
            dma((5, 2)),
            dma((5, 2)),
            dma((4, 2)),
            dma((4, 2)),
            dma((NTILE,)),
            dma((HALF + 1,)),
            dma((5,)),
            dma((4, 4)),
        ],
        compiler_params=pltpu.CompilerParams(collective_id=0, has_side_effects=True),
    )(logder)


def solution(mesh):
    torus = Mesh(mesh.devices.reshape(4, 8, 2, 4, 2), ("a", "z", "c", "x", "h"))
    return jax.shard_map(
        on_device,
        mesh=torus,
        in_specs=(P(("a", "z", "c"), ("x", "h")),),
        out_specs=P(("a", "z", "c"), None, ("x", "h"), None),
        check_vma=False,
    )
```
